32 devices in a mesh: gx: 8 (over z, y), gy: 4 (over x, core).
Axes of the slice: x: 2, y: 2, z: 4, core: 2. Of those that a mesh axis runs over, the one named last changes fastest.
Arguments:
- velocity: bfloat16 [3, 16, 16, 16, 512], P(None, 'gx', 'gy'), may hold values from -6 to 6
- part_pos: float32 [4096, 3, 128], P(('gx', 'gy')), may hold values from -1 to 1
- part_vel: float32 [4096, 3, 128], P(('gx', 'gy')), may hold values from -6 to 6
- part_coef: float32 [4096, 2, 128], P(('gx', 'gy')), may hold values from 0.3 to 3
- counts: int32 [4096], P(('gx', 'gy')), may hold values from 1 to 128
- dest: int32 [4096], P(('gx', 'gy')), may hold values from 0 to 3, as said below
- elem: int32 [4096], P(('gx', 'gy')), may hold values from 0 to 127, as said below
Outputs:
- drag: float32 [4096, 3, 128], P(('gx', 'gy'))
- source: float32 [3, 16, 16, 16, 512], P(None, 'gx', 'gy')
The draws below stay inside these ranges and needn't reach their ends.
Inputs may be any that keep to these rules, and one draw needn't show every extreme that they name: `dest`: every device sends exactly 32 blocks to each gy index. `elem`: on every owning device, each of its 128 elements receives exactly one block.
All inputs are finite; a program needn't handle non-finite values.
Results may differ from the reference program's by a relative error of at most 0.0003.
Values sent between devices are 32-bit elements; how exact they have to be, the bound alone decides.
A program may use at most 128 MiB of HBM per device.

```python
import math
import jax
import jax.numpy as jnp
from jax import lax

EXD = 2
EYD = 4
EZ = 16
NODES = 512
SLOTS = 128
E_DEV = 128
NEX = 16
NEY = 16
NB = 4096
N_GX = 8
N_GY = 4


def joint_routes(key):
    share_size = E_DEV // N_GY

    def one_row(row_key):
        elem_keys = jax.random.split(jax.random.fold_in(row_key, 1), N_GY)
        mix_keys = jax.random.split(jax.random.fold_in(row_key, 2), N_GY)
        ladder = jnp.arange(E_DEV, dtype=jnp.int32)
        incoming = jax.vmap(lambda k: jax.random.permutation(k, ladder))(elem_keys)
        elements = incoming.reshape(N_GY, N_GY, share_size).transpose(1, 0, 2).reshape(N_GY, E_DEV)
        targets = jnp.broadcast_to(jnp.arange(N_GY, dtype=jnp.int32)[None, :, None], (N_GY, N_GY, share_size)).reshape(N_GY, E_DEV)
        shuffle = jax.vmap(lambda k: jax.random.permutation(k, ladder))(mix_keys)
        return (jnp.take_along_axis(targets, shuffle, axis=1), jnp.take_along_axis(elements, shuffle, axis=1))
    targets, elements = jax.vmap(one_row)(jax.random.split(key, N_GX))
    return (targets.reshape(-1), elements.reshape(-1))


def draw_dest(key, part):
    return joint_routes(jax.random.fold_in(key, 7))[0]


def draw_elem(key, part):
    return joint_routes(jax.random.fold_in(key, 7))[1]


def set_ends(result, stream_key, low, high):
    extent = result.shape
    spot = [jax.random.randint(jax.random.fold_in(stream_key, axis), (), 0, extent[axis]) for axis in range(len(extent))]
    result = result.at[tuple(spot)].set(low)
    longest = extent.index(max(extent))
    spot[longest] = (spot[longest] + 1) % extent[longest]
    return result.at[tuple(spot)].set(high)


def block_scale(stream_key, extent, pieces, smallest, largest):
    def one(dim, parts):
        steps = jax.random.uniform(jax.random.fold_in(jax.random.fold_in(stream_key, 6), dim), (parts,), jnp.float32, smallest / len(pieces), largest / len(pieces))
        return jnp.repeat(jnp.exp(steps), extent[dim] // parts).reshape((-1,) + (1,) * (len(extent) - dim - 1))

    loudness = one(*pieces[0])
    for cut in pieces[1:]:
        loudness = loudness * one(*cut)
    return loudness


def scatter_about(key, shape, scale, most, cuts=(), kind=jnp.bfloat16):
    level = block_scale(key, shape, cuts, -0.22, 0.18) if cuts else 1.0
    drawn = jax.random.normal(key, shape, jnp.float32) * scale * level
    return jnp.minimum(jnp.maximum(drawn, -most), most).astype(kind)


def setup_inputs(seed: int = 0) -> dict:
    splits = jax.random.split(jax.random.key(seed), 8)
    return {
        "velocity": scatter_about(splits[0], (3, NEX, NEY, EZ, NODES), 1.0, 6.0, ((1, 8), (2, 4))),
        "part_pos": jnp.clip(jax.random.uniform(splits[1], (NB, 3, SLOTS), jnp.float32, -1.0, 1.0) * block_scale(splits[1], (NB, 3, SLOTS), ((0, 32),), -0.4, 0.0), -1.0, 1.0),
        "part_vel": scatter_about(splits[2], (NB, 3, SLOTS), 1.0, 6.0, ((0, 32),), jnp.float32),
        "part_coef": jnp.clip(jnp.exp(math.log(3.0) - 2.3025851 * jax.random.uniform(splits[3], (NB, 2, SLOTS), jnp.float32) ** block_scale(splits[3], (NB, 2, SLOTS), ((0, 32),), -0.2, 0.2)), 0.3, 3.0),
        "counts": set_ends(jax.random.randint(splits[4], (NB,), 1, 129), jax.random.fold_in(splits[4], 1), 1, 128).astype(jnp.int32),
        "dest": draw_dest(jax.random.fold_in(splits[7], 71), 0),
        "elem": draw_elem(jax.random.fold_in(splits[7], 71), 0),
    }


GLL = (-1.0, -0.8717401485096066, -0.5917001814331423, -0.2092992179024789, 0.2092992179024789, 0.5917001814331423, 0.8717401485096066, 1.0)
HIGH = lax.Precision.HIGHEST
SHARPNESS = 8.0

def lagrange_rows(coord):
    layers = []
    for i in range(8):
        product = jnp.ones_like(coord)
        for m in range(8):
            if m != i:
                product = product * ((coord - GLL[m]) / (GLL[i] - GLL[m]))
        layers.append(product)
    return jnp.stack(layers, axis=1)

def gauss_rows(coord, offset):
    points = jnp.array(GLL, dtype=jnp.float32)
    spacing = points[None, :, None] - (coord[:, None, :] + offset)
    return jnp.exp(-SHARPNESS * spacing * spacing)

def element_step(field, position, carried, coefs, filled):
    group = field.shape[0]
    width = position.shape[2]
    basis_r = lagrange_rows(position[:, 0])
    basis_s = lagrange_rows(position[:, 1])
    basis_t = lagrange_rows(position[:, 2])
    nodal = field.reshape(group, 3, 8, 64)
    partial_sum = jnp.einsum('gcia,gip->gcap', nodal, basis_r, precision=HIGH)
    planes = (basis_s[:, :, None, :] * basis_t[:, None, :, :]).reshape(group, 64, width)
    fluid = lax.optimization_barrier(jnp.sum(partial_sum * planes[:, None], axis=2))
    relative = fluid - carried
    speed = jnp.sqrt(lax.optimization_barrier(jnp.sum(relative * relative, axis=1)))
    factor = coefs[:, 0] * (1.0 + 0.15 * jnp.power(coefs[:, 1] * speed, 0.687))
    live = jnp.arange(width, dtype=jnp.int32)[None, :] < filled[:, None]
    drag = jnp.where(live[:, None, :], factor[:, None, :] * relative, jnp.zeros_like(relative))
    weights_s = gauss_rows(position[:, 1], 0.0)
    weights_t = gauss_rows(position[:, 2], 0.0)
    spread = (-drag)[:, :, None, None, :] * weights_s[:, None, :, None, :] * weights_t[:, None, None, :, :]
    spread = spread.reshape(group, 192, width)
    weights_r = jnp.stack([gauss_rows(position[:, 0], 0.0), gauss_rows(position[:, 0], 2.0), gauss_rows(position[:, 0], -2.0)], axis=1)
    deposit = jnp.einsum('gsip,gap->gsia', weights_r, spread, precision=HIGH)
    deposit = deposit.reshape(group, 3, 8, 3, 64).transpose(0, 1, 3, 2, 4).reshape(group, 3, 3, 512)
    return (drag, deposit)

def run_groups(field, position, carried, coefs, filled, group):
    total = field.shape[0]
    turns = total // group
    packed = tuple((a.reshape((turns, group) + a.shape[1:]) for a in (field, position, carried, coefs, filled)))
    drag, deposit = lax.map(lambda args: element_step(*args), packed)
    return (drag.reshape((total,) + drag.shape[2:]), deposit.reshape((total,) + deposit.shape[2:]))

def dss_axis(field, elem_axis, node_axis, far_lo, far_hi):
    count = field.shape[elem_axis]
    lower = lax.slice_in_dim(field, 0, 1, axis=node_axis)
    upper = lax.slice_in_dim(field, 7, 8, axis=node_axis)
    edge_shape = lax.slice_in_dim(lower, 0, 1, axis=elem_axis).shape
    lower_next = jnp.concatenate([lax.slice_in_dim(lower, 1, count, axis=elem_axis), far_lo.reshape(edge_shape)], axis=elem_axis)
    upper_prev = jnp.concatenate([far_hi.reshape(edge_shape), lax.slice_in_dim(upper, 0, count - 1, axis=elem_axis)], axis=elem_axis)
    middle = lax.slice_in_dim(field, 1, 7, axis=node_axis)
    return jnp.concatenate([lower + upper_prev, middle, upper + lower_next], axis=node_axis)

def edge_zeros(field, elem_axis, node_axis):
    edge = lax.slice_in_dim(lax.slice_in_dim(field, 0, 1, axis=elem_axis), 0, 1, axis=node_axis)
    return jnp.zeros_like(edge).reshape(-1)

def reference(velocity, part_pos, part_vel, part_coef, counts, dest, elem):
    blocks = part_pos.shape[0]
    source_row = jnp.arange(blocks, dtype=jnp.int32) // (E_DEV * N_GY)
    local_x = elem // (EYD * EZ)
    local_y = elem // EZ % EYD
    local_z = elem % EZ
    global_id = ((source_row * EXD + local_x) * NEY + dest * EYD + local_y) * EZ + local_z
    by_elem = jnp.argsort(global_id)
    field_e = velocity.reshape(3, blocks, NODES).transpose(1, 0, 2).astype(jnp.float32)
    drag_e, deposit = run_groups(field_e, part_pos[by_elem], part_vel[by_elem], part_coef[by_elem], counts[by_elem], math.gcd(blocks, 256))
    drag = drag_e[global_id]
    deposit = deposit.transpose(1, 2, 0, 3).reshape(3, 3, NEX, NEY, EZ, 8, 8, 8)
    own_part, minus_part, plus_part = (deposit[0], deposit[1], deposit[2])
    empty_layer = jnp.zeros_like(own_part[:, 0:1])
    total = own_part + jnp.concatenate([minus_part[:, 1:], empty_layer], axis=1) + jnp.concatenate([empty_layer, plus_part[:, :-1]], axis=1)
    field = total
    for elem_axis, node_axis in ((1, 4), (2, 5), (3, 6)):
        zeros_edge = edge_zeros(field, elem_axis, node_axis)
        field = dss_axis(field, elem_axis, node_axis, zeros_edge, zeros_edge)
    return (drag, field.reshape(3, NEX, NEY, EZ, NODES))
```

```python
import functools

import jax
import jax.numpy as jnp
from jax import lax
from jax.experimental import pallas as pl
from jax.experimental.pallas import tpu as pltpu
from jax.sharding import PartitionSpec as P

GLL = (
    -1.0,
    -0.8717401485096066,
    -0.5917001814331423,
    -0.2092992179024789,
    0.2092992179024789,
    0.5917001814331423,
    0.8717401485096066,
    1.0,
)
SHARPNESS = 8.0
VMEM = pltpu.VMEM
SMEM = pltpu.SMEM
ROWS = 24


def lane_iota(shape):
    return lax.broadcasted_iota(jnp.int32, shape, len(shape) - 1)


def node_consts():
    row = lax.broadcasted_iota(jnp.int32, (8, 128), 0)

    def pick(values):
        out = jnp.full((8, 128), values[7], jnp.float32)
        for i in range(7):
            out = jnp.where(row == i, jnp.float32(values[i]), out)
        return out

    others = [pick([[GLL[m] for m in range(8) if m != i][n] for i in range(8)]) for n in range(7)]
    scales = []
    for i in range(8):
        product = 1.0
        for m in range(8):
            if m != i:
                product *= GLL[i] - GLL[m]
        scales.append(1.0 / product)
    return pick(GLL), others, pick(scales)


def lagrange(x, others, scale):
    diffs = [x - o for o in others]
    left = (diffs[0] * diffs[1]) * (diffs[2] * diffs[3])
    right = (diffs[4] * diffs[5]) * (diffs[6] * scale)
    return left * right


def gauss(x, nodes):
    gap = nodes - x
    return jnp.exp(-SHARPNESS * gap * gap)


def split(x):
    high = x.astype(jnp.bfloat16)
    low = (x - high.astype(jnp.float32)).astype(jnp.bfloat16)
    return high, low


def planes(a, b):
    return jnp.concatenate([a[j : j + 1] * b for j in range(8)], axis=0)


def spread_nodes(vel_ref, vs_ref, elems):
    low = lane_iota((elems, 128)) < 64
    for c in range(3):
        for q in range(4):
            x = vel_ref[c, :, q * 128 : (q + 1) * 128].astype(jnp.float32)
            turned = pltpu.roll(x, 64, 1)
            vs_ref[pl.ds(c * 8 + 2 * q, elems, stride=ROWS), :] = jnp.where(low, x, turned)
            vs_ref[pl.ds(c * 8 + 2 * q + 1, elems, stride=ROWS), :] = jnp.where(low, turned, x)


def st_planes(s, t, nodes):
    high, low = split(planes(gauss(s, nodes), gauss(t, nodes)))
    gathered = jnp.concatenate([high, low], axis=0)
    return jnp.concatenate([gathered, gathered], axis=1)


def project(left, gathered):
    high, low = split(left)
    return lax.dot_general(
        jnp.concatenate([high, low], axis=1),
        gathered,
        (((1,), (1,)), ((), ())),
        preferred_element_type=jnp.float32,
    )


def element(block, count, field, consts, inner_minus, inner_plus):
    nodes, others, scale = consts
    r, s, t = (jnp.broadcast_to(block[d : d + 1], (8, 128)) for d in range(3))
    basis_r = lagrange(r, others, scale)
    basis_st = planes(lagrange(s, others, scale), lagrange(t, others, scale))
    high, low = split(basis_st)
    partial = jnp.dot(
        field.astype(jnp.bfloat16),
        jnp.concatenate([high, low], axis=0),
        preferred_element_type=jnp.float32,
    )
    rel = []
    for c in range(3):
        fluid = jnp.sum(partial[c * 8 : c * 8 + 8] * basis_r, axis=0, keepdims=True)
        rel.append(fluid - block[3 + c : 4 + c])
    speed = jnp.sqrt(rel[0] * rel[0] + rel[1] * rel[1] + rel[2] * rel[2])
    power = jnp.exp(0.687 * jnp.log(block[7:8] * speed))
    factor = block[6:7] * (1.0 + 0.15 * power)
    factor = jnp.where(lane_iota((1, 128)) < count, factor, 0.0)
    drag = [factor * w for w in rel]
    whole = jnp.concatenate(drag, axis=0)
    minus = gauss(r + 2.0, nodes)
    plus = gauss(r - 2.0, nodes)
    weights = [gauss(r, nodes)]
    if inner_minus:
        weights.append(minus)
    if inner_plus:
        weights.append(plus)
    rows = [(-d) * w for w in weights for d in drag]
    blank = jnp.zeros((5, 128), jnp.float32)
    if not inner_minus:
        rows.append(jnp.concatenate([-whole * minus[7:8], blank], axis=0))
    if not inner_plus:
        rows.append(jnp.concatenate([-whole * plus[0:1], blank], axis=0))
    out = project(jnp.concatenate(rows, axis=0), st_planes(s, t, nodes))
    parts, at = {}, ROWS
    parts["own"] = out[0:ROWS]
    for name, inner in (("minus", inner_minus), ("plus", inner_plus)):
        if inner:
            parts[name] = out[at : at + ROWS]
            at += ROWS
    for name, inner in (("minus", inner_minus), ("plus", inner_plus)):
        if not inner:
            parts[name] = out[at : at + 8]
            at += 8
    return whole, parts


def main_kernel(
    shape, chunks, n_gx, n_gy,
    slot_ref, count_ref, elem_ref, got_ref, vel_ref,
    field_ref, far_lo_ref, far_hi_ref, ret_ref,
    vs_ref, ts_ref, fs_ref, drag_ref, pos_ref, gpos_ref, gdrag_ref,
    face_ref, gface_ref, lo_ref, hi_ref, back_ref,
    pos_sem, drag_sem, face_sem, y_sem, back_sem,
):
    exd, eyd, ez = shape
    elems = exd * eyd * ez
    columns = eyd * ez
    share = elems // n_gy
    wide = columns // chunks
    group = min(8, wide)
    turns = columns // group
    per = turns // chunks
    half = columns // 2
    gx = lax.axis_index("gx")
    gy = lax.axis_index("gy")
    has = (gx > 0, gx < n_gx - 1)
    mesh_id = pl.DeviceIdType.MESH

    def to_side(side, src, dst, sems, *at):
        return pltpu.make_async_remote_copy(
            src_ref=src, dst_ref=dst,
            send_sem=sems.at[(0, side) + at], recv_sem=sems.at[(1, 1 - side) + at],
            device_id={"gx": gx - 1 if side == 0 else gx + 1}, device_id_type=mesh_id,
        )

    def from_side(side, src, dst, sems, *at):
        return pltpu.make_async_remote_copy(
            src_ref=src, dst_ref=dst,
            send_sem=sems.at[(0, side) + at], recv_sem=sems.at[(1, side) + at],
            device_id={"gx": gx - 1 if side == 0 else gx + 1}, device_id_type=mesh_id,
        )

    barrier = pltpu.get_barrier_semaphore()
    for side in range(2):
        @pl.when(has[side])
        def _():
            pl.semaphore_signal(
                barrier, inc=1, device_id={"gx": gx - 1 if side == 0 else gx + 1}, device_id_type=mesh_id
            )
    for off in range(1, n_gy):
        pl.semaphore_signal(
            barrier, inc=1, device_id={"gy": lax.rem(gy + off, n_gy)}, device_id_type=mesh_id
        )

    base = (0, elems - columns)

    def stage(index, carry):
        spots = [(side, index * 4 + u) for side in range(2) for u in range(4)]
        held = [got_ref[slot_ref[base[side] + col], 0:3] for side, col in spots]
        for (side, col), value in zip(spots, held):
            pos_ref[side, col] = value
        return carry

    lax.fori_loop(0, columns // 4, stage, 0)
    pl.semaphore_wait(
        barrier, n_gy - 1 + (gx > 0).astype(jnp.int32) + (gx < n_gx - 1).astype(jnp.int32)
    )
    for side in range(2):
        @pl.when(has[side])
        def _():
            to_side(side, pos_ref.at[side], gpos_ref.at[1 - side], pos_sem).start()

    spread_nodes(vel_ref, vs_ref, elems)
    consts = node_consts()
    nodes = consts[0]

    def drag_copy(make, side, chunk):
        start = base[side] + chunk * wide
        return make(
            side, drag_ref.at[pl.ds(start, wide)], gdrag_ref.at[1 - side, pl.ds(chunk * wide, wide)], drag_sem, chunk
        )

    def turn(index, carry):
        for g in range(group):
            col = index * group + g
            parts = []
            for x in range(exd):
                e = x * columns + col
                slot = slot_ref[e]
                drag, part = element(
                    got_ref[slot],
                    count_ref[slot],
                    vs_ref[pl.ds(pl.multiple_of(e * ROWS, 8), ROWS), :],
                    consts,
                    x > 0,
                    x + 1 < exd,
                )
                drag_ref[e] = drag
                parts.append(part)
            for x in range(exd):
                e = x * columns + col
                own = parts[x]["own"]
                if x + 1 < exd:
                    own = own + parts[x + 1]["minus"]
                if x > 0:
                    own = own + parts[x - 1]["plus"]
                ts_ref[pl.ds(pl.multiple_of(e * ROWS, 8), ROWS), :] = own
            start = pl.multiple_of(col * 8, 8)
            fs_ref[0, pl.ds(start, 8), :] = parts[0]["minus"]
            fs_ref[1, pl.ds(start, 8), :] = parts[exd - 1]["plus"]
        for side in range(2):
            @pl.when((lax.rem(index, per) == per - 1) & has[side])
            def _():
                drag_copy(to_side, side, lax.div(index, per)).start()
        return carry

    lax.fori_loop(0, turns, turn, 0)

    def doubled(x):
        return x + pltpu.roll(x, 64, 1)

    low_h = lane_iota((half, 128)) < 64
    for side in range(2):
        node = 0 if side == 0 else 7
        for c in range(3):
            one = doubled(ts_ref[pl.ds(base[side] * ROWS + c * 8 + node, half, stride=ROWS), :])
            two = doubled(ts_ref[pl.ds((base[side] + half) * ROWS + c * 8 + node, half, stride=ROWS), :])
            face_ref[side, c] = jnp.where(low_h, one, two)
        @pl.when(has[side])
        def _():
            to_side(side, face_ref.at[side], gface_ref.at[1 - side], face_sem).start()

    def fill(index, carry):
        held = [drag_ref[elem_ref[index * 8 + u]] for u in range(8)]
        for u in range(8):
            back_ref[index * 8 + u] = held[u]
        return carry

    lax.fori_loop(0, elems // 8, fill, 0)

    def back_copy(off):
        peer = lax.rem(gy + off, n_gy)
        return pltpu.make_async_remote_copy(
            src_ref=back_ref.at[pl.ds(peer * share, share)], dst_ref=ret_ref.at[pl.ds(gy * share, share)],
            send_sem=back_sem.at[0, off - 1], recv_sem=back_sem.at[1, off - 1],
            device_id={"gy": peer}, device_id_type=mesh_id,
        )

    for off in range(1, n_gy):
        back_copy(off).start()

    mine = pl.ds(gy * share, share)
    ret_ref[mine] = back_ref[mine]

    for side in range(2):
        @pl.when(has[side])
        def _():
            from_side(side, pos_ref.at[side], gpos_ref.at[side], pos_sem).wait()

        def ghost(chunk, carry):
            from_side(
                side, drag_ref.at[pl.ds(base[side] + chunk * wide, wide)],
                gdrag_ref.at[side, pl.ds(chunk * wide, wide)], drag_sem, chunk,
            ).wait()
            sums = []
            for g in range(wide):
                col = chunk * wide + g
                place = gpos_ref[side, col]
                force = gdrag_ref[side, col]
                r, s, t = (jnp.broadcast_to(place[d : d + 1], (8, 128)) for d in range(3))
                weight = gauss(r + (-2.0 if side == 0 else 2.0), nodes)
                rows = [(-force[c : c + 1]) * weight for c in range(3)]
                add = project(jnp.concatenate(rows, axis=0), st_planes(s, t, nodes))
                spot = pl.ds(pl.multiple_of((base[side] + col) * ROWS, 8), ROWS)
                sums.append((spot, ts_ref[spot, :] + add))
            for spot, value in sums:
                ts_ref[spot, :] = value
            return carry

        @pl.when(has[side])
        def _():
            lax.fori_loop(0, chunks, ghost, 0)

    for side in range(2):
        @pl.when(has[side])
        def _():
            from_side(side, face_ref.at[side], gface_ref.at[side], face_sem).wait()

    low = lane_iota((ez, 128)) < 64
    spot64 = lane_iota((ez, 128)) % 64

    def lanes(c, x, y, q):
        start = ((x * eyd + y) * ez) * ROWS + c * 8 + 2 * q
        even = ts_ref[pl.ds(start, ez, stride=ROWS), :]
        odd = ts_ref[pl.ds(start + 1, ez, stride=ROWS), :]
        return jnp.where(low, even, odd) + pltpu.roll(jnp.where(low, odd, even), 64, 1)

    def far(side, c, y):
        col = y * ez
        upper = col >= half
        row = col - half if upper else col
        came = gface_ref[side, c, row : row + ez, :]
        turned = pltpu.roll(came, 64, 1)
        came = jnp.where(low, turned, came) if upper else jnp.where(low, came, turned)
        mine = doubled(fs_ref[side, pl.ds(col * 8 + c, ez, stride=8), :])
        return jnp.where(has[side], came + mine, 0.0)

    for y in (0, eyd - 1) + tuple(range(1, eyd - 1)):
        for c in range(3):
            grid = [[lanes(c, x, y, q) for q in range(4)] for x in range(exd)]
            for x in range(exd):
                above = pltpu.roll(grid[x + 1][0], 64, 1) if x + 1 < exd else far(1, c, y)
                below = pltpu.roll(grid[x - 1][3], 64, 1) if x > 0 else far(0, c, y)
                done = list(grid[x])
                done[3] = done[3] + jnp.where(low, 0.0, above)
                done[0] = done[0] + jnp.where(low, below, 0.0)
                for q in range(4):
                    field_ref[c, x, y, :, q * 128 : (q + 1) * 128] = done[q]
                if y == 0:
                    face = jnp.where(spot64 < 8, done[0], 0.0)
                    for q in range(1, 4):
                        face = face + pltpu.roll(jnp.where(spot64 < 8, done[q], 0.0), 8 * q, 1)
                    lo_ref[c, x] = face
                if y == eyd - 1:
                    face = jnp.where(spot64 >= 56, done[0], 0.0)
                    for q in range(1, 4):
                        face = face + pltpu.roll(jnp.where(spot64 >= 56, done[q], 0.0), 128 - 8 * q, 1)
                    hi_ref[c, x] = face
        if y == eyd - 1:
            lo_copy = pltpu.make_async_remote_copy(
                src_ref=lo_ref, dst_ref=far_lo_ref, send_sem=y_sem.at[0, 0], recv_sem=y_sem.at[1, 0],
                device_id={"gy": gy - 1}, device_id_type=mesh_id,
            )
            hi_copy = pltpu.make_async_remote_copy(
                src_ref=hi_ref, dst_ref=far_hi_ref, send_sem=y_sem.at[0, 1], recv_sem=y_sem.at[1, 1],
                device_id={"gy": gy + 1}, device_id_type=mesh_id,
            )
            @pl.when(gy > 0)
            def _():
                lo_copy.start()
            @pl.when(gy < n_gy - 1)
            def _():
                hi_copy.start()

    @pl.when(gy > 0)
    def _():
        lo_copy.wait_send()
        hi_copy.wait_recv()
    @pl.when(gy < n_gy - 1)
    def _():
        hi_copy.wait_send()
        lo_copy.wait_recv()
    for off in range(1, n_gy):
        back_copy(off).wait()


def run_main(slot, count, elem_of, got, velocity, shape):
    exd, eyd, ez = shape
    elems = exd * eyd * ez
    columns = eyd * ez
    n_gx, n_gy = lax.axis_size("gx"), lax.axis_size("gy")
    chunks = 4
    f32 = jnp.float32
    dma = pltpu.SemaphoreType.DMA
    face = (3, exd, ez, 128)
    return pl.pallas_call(
        functools.partial(main_kernel, shape, chunks, n_gx, n_gy),
        out_shape=(
            jax.ShapeDtypeStruct((3, exd, eyd, ez, 512), f32),
            jax.ShapeDtypeStruct(face, f32),
            jax.ShapeDtypeStruct(face, f32),
            jax.ShapeDtypeStruct((elems, 3, 128), f32),
        ),
        in_specs=[pl.BlockSpec(memory_space=SMEM)] * 3 + [pl.BlockSpec(memory_space=VMEM)] * 2,
        out_specs=[pl.BlockSpec(memory_space=VMEM)] * 4,
        scratch_shapes=[
            pltpu.VMEM((elems * ROWS, 128), f32),
            pltpu.VMEM((elems * ROWS, 128), f32),
            pltpu.VMEM((2, columns * 8, 128), f32),
            pltpu.VMEM((elems, 3, 128), f32),
            pltpu.VMEM((2, columns, 3, 128), f32),
            pltpu.VMEM((2, columns, 3, 128), f32),
            pltpu.VMEM((2, columns, 3, 128), f32),
            pltpu.VMEM((2, 3, columns // 2, 128), f32),
            pltpu.VMEM((2, 3, columns // 2, 128), f32),
            pltpu.VMEM(face, f32),
            pltpu.VMEM(face, f32),
            pltpu.VMEM((elems, 3, 128), f32),
            dma((2, 2)),
            dma((2, 2, chunks)),
            dma((2, 2)),
            dma((2, 2)),
            dma((2, n_gy - 1)),
        ],
        compiler_params=pltpu.CompilerParams(
            vmem_limit_bytes=48 * 1024 * 1024, collective_id=0, has_side_effects=True
        ),
        cost_estimate=pl.CostEstimate(flops=200_000_000, bytes_accessed=4_000_000, transcendentals=700_000),
        name="elements",
    )(slot, count, elem_of, got, velocity)


def yz_pass(position_ref, field_ref, far_lo_ref, far_hi_ref, ret_ref, out_ref, drag_ref, buf_ref, sem):
    _, exd, eyd, ez, _ = field_ref.shape
    at = lax.axis_index("gy")
    first = at > 0
    last = at < lax.axis_size("gy") - 1
    place = lane_iota((ez, 128)) % 64
    k = lane_iota((ez, 128)) % 8
    row = lax.broadcasted_iota(jnp.int32, (ez, 128), 0)
    up = (k == 7) & (row < ez - 1)
    down = (k == 0) & (row > 0)

    def out_copy(c, x):
        return pltpu.make_async_copy(buf_ref.at[c, x], out_ref.at[c, x], sem.at[c, x])

    def layer(index, carry):
        c, x = lax.div(index, exd), lax.rem(index, exd)
        far_lo = jnp.where(last, far_lo_ref[c, x], 0.0)
        far_hi = jnp.where(first, far_hi_ref[c, x], 0.0)
        for q in range(4):
            spot = slice(q * 128, (q + 1) * 128)
            cells = [field_ref[c, x, y, :, spot] for y in range(eyd)]
            for y in range(eyd):
                if y + 1 < eyd:
                    above = pltpu.roll(cells[y + 1], 56, 1)
                else:
                    above = pltpu.roll(far_lo, (56 - 8 * q) % 128, 1)
                if y > 0:
                    below = pltpu.roll(cells[y - 1], 72, 1)
                else:
                    below = pltpu.roll(far_hi, (72 + 8 * q) % 128, 1)
                v = cells[y] + jnp.where(place >= 56, above, 0.0) + jnp.where(place < 8, below, 0.0)
                nxt = pltpu.roll(pltpu.roll(v, ez - 1, 0), 7, 1)
                prv = pltpu.roll(pltpu.roll(v, 1, 0), 121, 1)
                buf_ref[c, x, y, :, spot] = v + jnp.where(up, nxt, 0.0) + jnp.where(down, prv, 0.0)
        out_copy(c, x).start()
        return carry

    lax.fori_loop(0, 3 * exd, layer, 0)

    def pick(index, carry):
        held = [ret_ref[position_ref[index * 8 + u]] for u in range(8)]
        for c in range(3):
            rows = jnp.concatenate([h[c : c + 1] for h in held], axis=0)
            drag_ref[c, pl.ds(pl.multiple_of(index * 8, 8), 8), :] = rows
        return carry

    lax.fori_loop(0, ret_ref.shape[0] // 8, pick, 0)

    def drain(index, carry):
        out_copy(lax.div(index, exd), lax.rem(index, exd)).wait()
        return carry

    lax.fori_loop(0, 3 * exd, drain, 0)


def run_yz(position, field, far_lo, far_hi, ret):
    f32 = jnp.float32
    return pl.pallas_call(
        yz_pass,
        out_shape=(jax.ShapeDtypeStruct(field.shape, f32), jax.ShapeDtypeStruct((3, ret.shape[0], 128), f32)),
        in_specs=[pl.BlockSpec(memory_space=SMEM)] + [pl.BlockSpec(memory_space=VMEM)] * 4,
        out_specs=[pl.BlockSpec(memory_space=pl.ANY), pl.BlockSpec(memory_space=VMEM)],
        scratch_shapes=[pltpu.VMEM(field.shape, f32), pltpu.SemaphoreType.DMA(field.shape[:2])],
        compiler_params=pltpu.CompilerParams(vmem_limit_bytes=32 * 1024 * 1024),
        name="yzpass",
    )(position, field, far_lo, far_hi, ret)


def send_kernel(
    n_gy, sorting_ref, pos_hbm, vel_hbm, coef_hbm, label_ref,
    got_ref, got_label_ref, pos_ref, vel_ref, coef_ref, send_ref, sem, label_sem, in_sem,
):
    pairs = ((pos_hbm, pos_ref), (vel_hbm, vel_ref), (coef_hbm, coef_ref))
    inputs = [pltpu.make_async_copy(src, dst, in_sem.at[i]) for i, (src, dst) in enumerate(pairs)]
    for copy in inputs:
        copy.start()
    share = pos_ref.shape[1] // n_gy
    gy = lax.axis_index("gy")
    mesh_id = pl.DeviceIdType.MESH
    barrier = pltpu.get_barrier_semaphore()
    for off in range(1, n_gy):
        pl.semaphore_signal(
            barrier, inc=1, device_id={"gy": lax.rem(gy + off, n_gy)}, device_id_type=mesh_id
        )

    def block_copy(off):
        peer = lax.rem(gy + off, n_gy)
        return pltpu.make_async_remote_copy(
            src_ref=send_ref.at[pl.ds(peer * share, share)], dst_ref=got_ref.at[pl.ds(gy * share, share)],
            send_sem=sem.at[0, off - 1], recv_sem=sem.at[1, off - 1],
            device_id={"gy": peer}, device_id_type=mesh_id,
        )

    def label_copy(off):
        peer = lax.rem(gy + off, n_gy)
        return pltpu.make_async_remote_copy(
            src_ref=label_ref.at[peer], dst_ref=got_label_ref.at[gy],
            send_sem=label_sem.at[0, off - 1], recv_sem=label_sem.at[1, off - 1],
            device_id={"gy": peer}, device_id_type=mesh_id,
        )

    def pack(dst, start):
        def some(index, carry):
            held = []
            for u in range(4):
                b = sorting_ref[start + index * 4 + u]
                rows = [ref[c, pl.ds(b, 1), :] for ref in (pos_ref, vel_ref) for c in range(3)]
                held.append(jnp.concatenate(rows + [coef_ref[b]], axis=0))
            for u in range(4):
                dst[start + index * 4 + u] = held[u]
            return carry

        lax.fori_loop(0, share // 4, some, 0)

    order = sorted(range(1, n_gy), key=lambda off: -min(off, n_gy - off))
    for copy in inputs:
        copy.wait()
    for place, off in enumerate(order):
        pack(send_ref, lax.rem(gy + off, n_gy) * share)
        if place == 0:
            pl.semaphore_wait(barrier, n_gy - 1)
            for other in order:
                label_copy(other).start()
        block_copy(off).start()
    pack(got_ref, gy * share)
    got_label_ref[gy] = label_ref[gy]
    for off in order:
        label_copy(off).wait()
    for off in order:
        block_copy(off).wait()


def run_send(sorting, pos, vel, coef, label):
    n_gy = lax.axis_size("gy")
    elems = pos.shape[1]
    f32 = jnp.float32
    dma = pltpu.SemaphoreType.DMA
    return pl.pallas_call(
        functools.partial(send_kernel, n_gy),
        out_shape=(
            jax.ShapeDtypeStruct((elems, 8, 128), f32),
            jax.ShapeDtypeStruct(label.shape, f32),
        ),
        in_specs=[pl.BlockSpec(memory_space=SMEM)]
        + [pl.BlockSpec(memory_space=pltpu.HBM)] * 3
        + [pl.BlockSpec(memory_space=VMEM)],
        out_specs=[pl.BlockSpec(memory_space=VMEM)] * 2,
        scratch_shapes=[
            pltpu.VMEM(pos.shape, f32),
            pltpu.VMEM(vel.shape, f32),
            pltpu.VMEM(coef.shape, f32),
            pltpu.VMEM((elems, 8, 128), f32),
            dma((2, n_gy - 1)),
            dma((2, n_gy - 1)),
            dma((3,)),
        ],
        compiler_params=pltpu.CompilerParams(
            vmem_limit_bytes=32 * 1024 * 1024, collective_id=1, has_side_effects=True
        ),
        name="migrate",
    )(sorting, *(pltpu.with_memory_space_constraint(x, pltpu.HBM) for x in (pos, vel, coef)), label)


def inverse_of(position):
    n = position.shape[0]
    ladder = jnp.arange(n, dtype=jnp.int32)
    return jnp.sum(jnp.where(position[None, :] == ladder[:, None], ladder[None, :], 0), axis=1)


def body(velocity, part_pos, part_vel, part_coef, counts, dest, elem):
    _, exd, eyd, ez, nodes = velocity.shape
    elems = exd * eyd * ez
    devices = lax.axis_size("gy")
    share = elems // devices
    f32 = jnp.float32
    ladder = jnp.arange(elems, dtype=jnp.int32)
    earlier = (dest[None, :] == dest[:, None]) & (ladder[None, :] < ladder[:, None])
    position = dest * share + jnp.sum(earlier.astype(jnp.int32), axis=1)
    sorting = inverse_of(position)
    lanes = max(128, share)
    tags = elem * 256 + counts
    room = (position // share) * lanes + position % share
    cells = jnp.arange(devices * lanes, dtype=jnp.int32)
    label = jnp.sum(jnp.where(room[None, :] == cells[:, None], tags[None, :], 0), axis=1)
    got, got_label = run_send(
        sorting, part_pos.transpose(1, 0, 2), part_vel.transpose(1, 0, 2), part_coef,
        label.astype(f32).reshape(devices, 1, lanes),
    )
    got_labels = got_label[:, 0, :share].reshape(elems).astype(jnp.int32)
    slot = inverse_of(got_labels // 256)
    field, far_lo, far_hi, ret = run_main(
        slot, got_labels % 256, got_labels // 256, got,
        velocity.reshape(3, elems, nodes), (exd, eyd, ez),
    )
    source, drag_out = run_yz(position, field, far_lo, far_hi, ret)
    return (drag_out.transpose(1, 0, 2), source)


def solution(mesh):
    in_specs = (
        P(None, "gx", "gy", None, None),
        P(("gx", "gy"), None, None),
        P(("gx", "gy"), None, None),
        P(("gx", "gy"), None, None),
        P(("gx", "gy")),
        P(("gx", "gy")),
        P(("gx", "gy")),
    )
    out_specs = (P(("gx", "gy"), None, None), P(None, "gx", "gy", None, None))
    return jax.shard_map(body, mesh=mesh, in_specs=in_specs, out_specs=out_specs, check_vma=False)
```

```python
import functools
import math

import jax
import jax.numpy as jnp
from jax import lax
from jax.experimental import pallas as pl
from jax.experimental.pallas import tpu as pltpu
from jax.sharding import PartitionSpec as P

GLL = (
    -1.0,
    -0.8717401485096066,
    -0.5917001814331423,
    -0.2092992179024789,
    0.2092992179024789,
    0.5917001814331423,
    0.8717401485096066,
    1.0,
)
SHARPNESS = 8.0
WIDTH = math.sqrt(SHARPNESS * math.log2(math.e))
VMEM = pltpu.VMEM
SMEM = pltpu.SMEM
ROWS = 24


def lane_iota(shape):
    return lax.broadcasted_iota(jnp.int32, shape, len(shape) - 1)


def node_consts():
    row = lax.broadcasted_iota(jnp.int32, (8, 128), 0)

    def pick(values):
        out = jnp.full((8, 128), values[7], jnp.float32)
        for i in range(7):
            out = jnp.where(row == i, jnp.float32(values[i]), out)
        return out

    others = [pick([[GLL[m] for m in range(8) if m != i][n] for i in range(8)]) for n in range(7)]
    scales = []
    for i in range(8):
        product = 1.0
        for m in range(8):
            if m != i:
                product *= GLL[i] - GLL[m]
        scales.append(1.0 / product)
    return pick(GLL), others, pick(scales)


def lagrange(x, others, scale):
    diffs = [x - o for o in others]
    left = (diffs[0] * diffs[1]) * (diffs[2] * diffs[3])
    right = (diffs[4] * diffs[5]) * (diffs[6] * scale)
    return left * right


def gauss(x, nodes):
    gap = nodes - x
    return jnp.exp2(-(gap * gap))


def split(x):
    high = x.astype(jnp.bfloat16)
    low = (x - high.astype(jnp.float32)).astype(jnp.bfloat16)
    return high, low


def planes(a, b):
    return jnp.concatenate([a[j : j + 1] * b for j in range(8)], axis=0)


def spread_nodes(vel_ref, vs_ref, elems):
    low = lane_iota((elems, 128)) < 64
    for c in range(3):
        for q in range(4):
            x = vel_ref[c, :, q * 128 : (q + 1) * 128].astype(jnp.float32)
            turned = pltpu.roll(x, 64, 1)
            vs_ref[pl.ds(c * 8 + 2 * q, elems, stride=ROWS), :] = jnp.where(low, x, turned)
            vs_ref[pl.ds(c * 8 + 2 * q + 1, elems, stride=ROWS), :] = jnp.where(low, turned, x)


def rows_of(refs):
    return jnp.concatenate(refs, axis=0)


def project(left, high, low):
    top, rest = split(left)
    both = jnp.concatenate([jnp.concatenate([top, top], axis=1), jnp.concatenate([rest, rest], axis=1)], axis=0)
    out = lax.dot_general(
        both, jnp.concatenate([high, low], axis=1), (((1,), (1,)), ((), ())), preferred_element_type=jnp.float32
    )
    return out[: left.shape[0]] + out[left.shape[0] :]


def st_planes(s, t, nodes):
    return split(planes(gauss(s, nodes), gauss(t, nodes)))


def line(ref, c, at):
    return ref[c, pl.ds(at, 1), :]


def wide_line(ref, c, at):
    return jnp.broadcast_to(line(ref, c, at), (8, 128))


def main_kernel(
    shape, n_gx, n_gy,
    sorting_ref, count_ref, label_ref, pos_hbm, vel_hbm, coef_hbm, velocity_hbm,
    field_ref, far_lo_ref, far_hi_ref, ret_ref,
    pos_in, vel_in, coef_in, vel_ref, send_pos, send_rest, got_pos, got_rest, got_label, slot_row, tag_s, slot_s,
    vs_ref, fluid_ref, drag_ref, dep_ref, ts_ref, fs_ref,
    pos_ref, gpos_ref, out_ref, gdrag_ref, face_ref, gface_ref, lo_ref, hi_ref,
    in_sem, label_sem, block_sem, rest_sem, tag_sem, pos_sem, drag_sem, face_sem, y_sem, back_sem,
):
    exd, eyd, ez = shape
    elems = exd * eyd * ez
    columns = eyd * ez
    share = elems // n_gy
    half = columns // 2
    group = 16
    per = share // group
    near = n_gy // 2
    i32 = jnp.int32
    gx = lax.axis_index("gx")
    gy = lax.axis_index("gy")
    has = (gx > 0, gx < n_gx - 1)
    mesh_id = pl.DeviceIdType.MESH

    def partner(m):
        total, bit = 0, 1
        while bit < n_gy:
            total = total + lax.rem(lax.div(gy, bit) + lax.div(m, bit), 2) * bit
            bit *= 2
        return total

    pairs = ((pos_hbm, pos_in), (vel_hbm, vel_in), (coef_hbm, coef_in), (velocity_hbm, vel_ref))
    inputs = [pltpu.make_async_copy(src, dst, in_sem.at[i]) for i, (src, dst) in enumerate(pairs)]
    for copy in inputs:
        copy.start()

    def side_id(side):
        return {"gx": gx - 1 if side == 0 else gx + 1}

    def to_side(side, src, dst, sems, *at):
        return pltpu.make_async_remote_copy(
            src_ref=src, dst_ref=dst, send_sem=sems.at[(0, side) + at], recv_sem=sems.at[(1, 1 - side) + at],
            device_id=side_id(side), device_id_type=mesh_id,
        )

    def from_side(side, src, dst, sems, *at):
        return pltpu.make_async_remote_copy(
            src_ref=src, dst_ref=dst, send_sem=sems.at[(0, side) + at], recv_sem=sems.at[(1, side) + at],
            device_id=side_id(side), device_id_type=mesh_id,
        )

    barrier = pltpu.get_barrier_semaphore()
    for side in range(2):
        @pl.when(has[side])
        def _():
            pl.semaphore_signal(barrier, inc=1, device_id=side_id(side), device_id_type=mesh_id)
    for m in range(1, n_gy):
        pl.semaphore_signal(barrier, inc=1, device_id={"gy": partner(m)}, device_id_type=mesh_id)

    def peer_copy(src, dst, sems, m):
        return pltpu.make_async_remote_copy(
            src_ref=src, dst_ref=dst, send_sem=sems.at[0, m - 1], recv_sem=sems.at[1, m - 1],
            device_id={"gy": partner(m)}, device_id_type=mesh_id,
        )

    def part(index):
        return pl.ds(pl.multiple_of(index * share, 8), share)

    def label_copy(m):
        return peer_copy(label_ref.at[partner(m)], got_label.at[gy], label_sem, m)

    def pos_copy(m):
        return peer_copy(send_pos.at[:, part(partner(m))], got_pos.at[:, part(gy)], block_sem, m)

    def rest_copy(m):
        return peer_copy(send_rest.at[:, part(partner(m))], got_rest.at[:, part(gy)], rest_sem, m)

    def back_copy(m):
        return peer_copy(drag_ref.at[:, part(partner(m))], ret_ref.at[:, part(gy)], back_sem, m)

    def tag_copy(index, m):
        return pltpu.make_async_copy(got_label.at[index], tag_s.at[index], tag_sem.at[m])

    lane = lane_iota((1, 128))

    def pack_pos(dst, index):
        def some(i, carry):
            start = pl.multiple_of(index * share + i * 8, 8)
            spots = [sorting_ref[start + u] for u in range(8)]
            for c in range(3):
                dst[c, pl.ds(start, 8), :] = rows_of([line(pos_in, c, b) for b in spots])
            return carry

        lax.fori_loop(0, share // 8, some, 0)

    def pack_rest(dst, index):
        def some(i, carry):
            start = pl.multiple_of(index * share + i * 8, 8)
            spots = [sorting_ref[start + u] for u in range(8)]
            for c in range(3):
                dst[c, pl.ds(start, 8), :] = rows_of([line(vel_in, c, b) for b in spots])
            dst[3, pl.ds(start, 8), :] = rows_of(
                [jnp.where(lane < count_ref[b], coef_in[b, 0:1, :], 0.0) for b in spots]
            )
            dst[4, pl.ds(start, 8), :] = rows_of([coef_in[b, 1:2, :] for b in spots])
            return carry

        lax.fori_loop(0, share // 8, some, 0)

    got_label[gy] = label_ref[gy]
    tag_copy(gy, 0).start()
    order = tuple(range(near, n_gy)) + tuple(range(1, near))
    inputs[0].wait()
    for m in order[: n_gy - near]:
        pack_pos(send_pos, partner(m))
    pl.semaphore_wait(barrier, n_gy - 1 + has[0].astype(i32) + has[1].astype(i32))
    for m in order:
        label_copy(m).start()
    for m in order[: n_gy - near]:
        pos_copy(m).start()
    inputs[1].wait()
    inputs[2].wait()
    for m in order[: n_gy - near]:
        pack_rest(send_rest, partner(m))
        rest_copy(m).start()
    for m in order[n_gy - near :]:
        pack_pos(send_pos, partner(m))
        pos_copy(m).start()
        pack_rest(send_rest, partner(m))
        rest_copy(m).start()
    pack_pos(got_pos, gy)
    pack_rest(got_rest, gy)
    inputs[3].wait()
    spread_nodes(vel_ref, vs_ref, elems)
    consts = node_consts()
    nodes, others, scale = consts
    nodes = nodes * WIDTH
    tag_copy(gy, 0).wait()

    def slot_of(e):
        return slot_s[0, e]

    def collect(dst, src, start, count):
        def some(i, carry):
            for side in range(2):
                at = pl.multiple_of(start + i * 8, 8)
                spots = [slot_of(side * columns + at + u) for u in range(8)]
                for c in range(3):
                    dst[side, c, pl.ds(at, 8), :] = rows_of([line(src, c, b) for b in spots])
            return carry

        lax.fori_loop(0, count // 8, some, 0)

    def interpolate(index, carry):
        for m in range(1, near):
            @pl.when(index == m * per)
            def _():
                label_copy(m).wait()
                tag_copy(partner(m), m).start()
                pos_copy(m).wait()
                tag_copy(partner(m), m).wait()

        @pl.when(index == near * per)
        def _():
            for m in range(near, n_gy):
                label_copy(m).wait()
                tag_copy(partner(m), m).start()
            total = got_label[0]
            for other in range(1, n_gy):
                total = total + got_label[other]
            slot_row[...] = total[:, 128:]
            copy = pltpu.make_async_copy(slot_row, slot_s, tag_sem.at[n_gy])
            copy.start()
            for m in range(near, n_gy):
                tag_copy(partner(m), m).wait()
            copy.wait()
            for m in range(near, n_gy):
                pos_copy(m).wait()
            collect(pos_ref, got_pos, 0, columns)
            for side in range(2):
                @pl.when(has[side])
                def _():
                    to_side(side, pos_ref.at[side], gpos_ref.at[1 - side], pos_sem).start()

        source = partner(lax.div(index, per))
        first = lax.rem(index, per) * group
        for batch in range(group // 8):
            fluid = [[], [], []]
            for u in range(8):
                i = first + batch * 8 + u
                slot = source * share + i
                e = tag_s[source, 0, i]
                r, s, t = (wide_line(got_pos, d, slot) for d in range(3))
                basis_r = lagrange(r, others, scale)
                high, low = split(planes(lagrange(s, others, scale), lagrange(t, others, scale)))
                partial = jnp.dot(
                    vs_ref[pl.ds(e * ROWS, ROWS), :].astype(jnp.bfloat16),
                    jnp.concatenate([high, low], axis=0),
                    preferred_element_type=jnp.float32,
                )
                for c in range(3):
                    fluid[c].append(jnp.sum(partial[c * 8 : c * 8 + 8] * basis_r, axis=0, keepdims=True))
            at = pl.multiple_of(source * share + first + batch * 8, 8)
            for c in range(3):
                fluid_ref[c, pl.ds(at, 8), :] = rows_of(fluid[c])
        return carry

    lax.fori_loop(0, elems // group, interpolate, 0)

    def forces(start, count):
        def some(i, carry):
            m = lax.div(start + i * 8, share)
            at = pl.ds(pl.multiple_of(partner(m) * share + lax.rem(start + i * 8, share), 8), 8)
            rel = [fluid_ref[c, at, :] - got_rest[c, at, :] for c in range(3)]
            speed = jnp.sqrt(rel[0] * rel[0] + rel[1] * rel[1] + rel[2] * rel[2])
            power = jnp.exp(0.687 * jnp.log(got_rest[4, at, :] * speed))
            factor = got_rest[3, at, :] * (1.0 + 0.15 * power)
            for c in range(3):
                drag_ref[c, at, :] = factor * rel[c]
            return carry

        lax.fori_loop(0, count // 8, some, 0)

    def strip(k):
        return lax.rem(k * (eyd - 1), eyd)

    def drag_copy(make, side, y):
        at = pl.ds(pl.multiple_of(y * ez, 8), ez)
        return make(side, out_ref.at[side, :, at], gdrag_ref.at[1 - side, :, at], drag_sem, y)

    def deposit(index, carry):
        @pl.when(index == 0)
        def _():
            for m in range(1, near):
                rest_copy(m).wait()
            forces(0, near * share)

        @pl.when(index == near * per)
        def _():
            for m in range(near, n_gy):
                rest_copy(m).wait()
            forces(near * share, elems - near * share)
            for k in range(eyd):
                y = k * (eyd - 1) % eyd
                collect(out_ref, drag_ref, y * ez, ez)
                for side in range(2):
                    @pl.when(has[side])
                    def _():
                        drag_copy(to_side, side, y).start()
            for m in order:
                back_copy(m).start()
            ret_ref[:, part(gy), :] = drag_ref[:, part(gy), :]

        source = partner(lax.div(index, per))
        first = lax.rem(index, per) * group
        for u in range(group):
            i = first + u
            slot = source * share + i
            layer = jnp.full((8, 128), tag_s[source, 0, i], i32)
            shift = jnp.where(layer < columns, -2.0 * WIDTH, 2.0 * WIDTH)
            r, s, t = (wide_line(got_pos, d, slot) * WIDTH for d in range(3))
            weights = (gauss(r, nodes), gauss(r + shift, nodes))
            force = [-line(drag_ref, c, slot) for c in range(3)]
            left = jnp.concatenate([f * w for w in weights for f in force], axis=0)
            out = project(left, *st_planes(s, t, nodes))
            dep_ref[pl.ds(pl.multiple_of(slot * 2 * ROWS, 8), 2 * ROWS), 0:64] = out
        return carry

    lax.fori_loop(0, elems // group, deposit, 0)

    def gather(i, carry):
        for side in range(exd):
            spots = []
            for u in range(8):
                col = i * 8 + u
                mine = slot_of(side * columns + col) * (2 * ROWS)
                other = slot_of((1 - side) * columns + col) * (2 * ROWS) + ROWS
                e = side * columns + col
                ts_ref[pl.ds(pl.multiple_of(e * ROWS, 8), ROWS), :] = (
                    dep_ref[pl.ds(mine, ROWS), :] + dep_ref[pl.ds(other, ROWS), :]
                )
                spots.append(mine)
            node = 0 if side == 0 else 7
            for c in range(3):
                fs_ref[side, c, pl.ds(pl.multiple_of(i * 8, 8), 8), :] = rows_of(
                    [dep_ref[pl.ds(at + c * 8 + node, 1), :] for at in spots]
                )
        return carry

    lax.fori_loop(0, columns // 8, gather, 0)

    base = (0, elems - columns)
    low_h = lane_iota((half, 128)) < 64
    for side in range(2):
        node = 0 if side == 0 else 7
        for c in range(3):
            one = ts_ref[pl.ds(base[side] * ROWS + c * 8 + node, half, stride=ROWS), :]
            two = ts_ref[pl.ds((base[side] + half) * ROWS + c * 8 + node, half, stride=ROWS), :]
            face_ref[side, c] = jnp.where(low_h, one, pltpu.roll(two, 64, 1))
        @pl.when(has[side])
        def _():
            to_side(side, face_ref.at[side], gface_ref.at[1 - side], face_sem).start()

    for side in range(2):
        @pl.when(has[side])
        def _():
            from_side(side, pos_ref.at[side], gpos_ref.at[side], pos_sem).wait()

    def ghost(k, carry):
        y = strip(k)
        for side in range(2):
            @pl.when(has[side])
            def _():
                at = pl.ds(pl.multiple_of(y * ez, 8), ez)
                from_side(side, out_ref.at[side, :, at], gdrag_ref.at[side, :, at], drag_sem, y).wait()
                sums = []
                for g in range(ez):
                    col = y * ez + g
                    r, s, t = (jnp.broadcast_to(gpos_ref[side, d, pl.ds(col, 1), :], (8, 128)) * WIDTH for d in range(3))
                    weight = gauss(r + (-2.0 if side == 0 else 2.0) * WIDTH, nodes)
                    left = jnp.concatenate([(-gdrag_ref[side, c, pl.ds(col, 1), :]) * weight for c in range(3)], axis=0)
                    add = project(left, *st_planes(s, t, nodes))
                    spot = pl.ds(pl.multiple_of((base[side] + col) * ROWS, 8), ROWS)
                    sums.append((spot, ts_ref[spot, 0:64] + add))
                for spot, value in sums:
                    ts_ref[spot, 0:64] = value
        return carry

    lax.fori_loop(0, eyd, ghost, 0)

    for side in range(2):
        @pl.when(has[side])
        def _():
            from_side(side, face_ref.at[side], gface_ref.at[side], face_sem).wait()

    low = lane_iota((ez, 128)) < 64
    spot64 = lane_iota((ez, 128)) % 64
    lo_copy = pltpu.make_async_remote_copy(
        src_ref=lo_ref, dst_ref=far_lo_ref, send_sem=y_sem.at[0, 0], recv_sem=y_sem.at[1, 0],
        device_id={"gy": gy - 1}, device_id_type=mesh_id,
    )
    hi_copy = pltpu.make_async_remote_copy(
        src_ref=hi_ref, dst_ref=far_hi_ref, send_sem=y_sem.at[0, 1], recv_sem=y_sem.at[1, 1],
        device_id={"gy": gy + 1}, device_id_type=mesh_id,
    )

    def assemble(index, carry):
        k, c = lax.div(index, 3), lax.rem(index, 3)
        y = strip(k)
        upper = y >= eyd // 2

        def lanes(x, q):
            start = (x * columns + y * ez) * ROWS + c * 8 + 2 * q
            even = ts_ref[pl.ds(start, ez, stride=ROWS), :]
            odd = ts_ref[pl.ds(start + 1, ez, stride=ROWS), :]
            return jnp.where(low, even, pltpu.roll(odd, 64, 1))

        def far(side):
            came = gface_ref[side, c, pl.ds(pl.multiple_of(lax.rem(y, eyd // 2) * ez, 8), ez), :]
            turned = pltpu.roll(came, 64, 1)
            came = jnp.where(low != upper, came, turned)
            mine = fs_ref[side, c, pl.ds(pl.multiple_of(y * ez, 8), ez), :]
            mine = jnp.where(low, mine, pltpu.roll(mine, 64, 1))
            return jnp.where(has[side], came + mine, 0.0)

        grid = [[lanes(x, q) for q in range(4)] for x in range(exd)]
        for x in range(exd):
            above = pltpu.roll(grid[x + 1][0], 64, 1) if x + 1 < exd else far(1)
            below = pltpu.roll(grid[x - 1][3], 64, 1) if x > 0 else far(0)
            done = list(grid[x])
            done[3] = done[3] + jnp.where(low, 0.0, above)
            done[0] = done[0] + jnp.where(low, below, 0.0)
            for q in range(4):
                field_ref[c, x, y, :, q * 128 : (q + 1) * 128] = done[q]

            @pl.when(k == 0)
            def _():
                face = jnp.where(spot64 < 8, done[0], 0.0)
                for q in range(1, 4):
                    face = face + pltpu.roll(jnp.where(spot64 < 8, done[q], 0.0), 8 * q, 1)
                lo_ref[c, x] = face

            @pl.when(k == 1)
            def _():
                face = jnp.where(spot64 >= 56, done[0], 0.0)
                for q in range(1, 4):
                    face = face + pltpu.roll(jnp.where(spot64 >= 56, done[q], 0.0), 128 - 8 * q, 1)
                hi_ref[c, x] = face

        @pl.when((index == 2) & (gy > 0))
        def _():
            lo_copy.start()

        @pl.when((index == 5) & (gy < n_gy - 1))
        def _():
            hi_copy.start()

        return carry

    lax.fori_loop(0, 3 * eyd, assemble, 0)

    @pl.when(gy > 0)
    def _():
        lo_copy.wait_send()
        hi_copy.wait_recv()

    @pl.when(gy < n_gy - 1)
    def _():
        hi_copy.wait_send()
        lo_copy.wait_recv()

    for m in order:
        back_copy(m).wait()


def run_main(sorting, counts, label, pos, vel, coef, velocity, shape):
    exd, eyd, ez = shape
    elems = exd * eyd * ez
    columns = eyd * ez
    n_gx, n_gy = lax.axis_size("gx"), lax.axis_size("gy")
    f32, i32 = jnp.float32, jnp.int32
    dma = pltpu.SemaphoreType.DMA
    face = (3, exd, ez, 128)
    strips = (2, 3, columns, 128)
    hbm = [pltpu.with_memory_space_constraint(x, pltpu.HBM) for x in (pos, vel, coef, velocity)]
    return pl.pallas_call(
        functools.partial(main_kernel, shape, n_gx, n_gy),
        out_shape=(
            jax.ShapeDtypeStruct((3, exd, eyd, ez, 512), f32),
            jax.ShapeDtypeStruct(face, f32),
            jax.ShapeDtypeStruct(face, f32),
            jax.ShapeDtypeStruct((3, elems, 128), f32),
        ),
        in_specs=[pl.BlockSpec(memory_space=SMEM)] * 2
        + [pl.BlockSpec(memory_space=VMEM)]
        + [pl.BlockSpec(memory_space=pltpu.HBM)] * 4,
        out_specs=[pl.BlockSpec(memory_space=VMEM)] * 4,
        scratch_shapes=[
            pltpu.VMEM(pos.shape, f32),
            pltpu.VMEM(vel.shape, f32),
            pltpu.VMEM(coef.shape, f32),
            pltpu.VMEM(velocity.shape, velocity.dtype),
            pltpu.VMEM((3, elems, 128), f32),
            pltpu.VMEM((5, elems, 128), f32),
            pltpu.VMEM((3, elems, 128), f32),
            pltpu.VMEM((5, elems, 128), f32),
            pltpu.VMEM(label.shape, i32),
            pltpu.VMEM((1, 128), i32),
            pltpu.SMEM(label.shape, i32),
            pltpu.SMEM((1, 128), i32),
            pltpu.VMEM((elems * ROWS, 128), f32),
            pltpu.VMEM((3, elems, 128), f32),
            pltpu.VMEM((3, elems, 128), f32),
            pltpu.VMEM((elems * 2 * ROWS, 128), f32),
            pltpu.VMEM((elems * ROWS, 128), f32),
            pltpu.VMEM(strips, f32),
            pltpu.VMEM(strips, f32),
            pltpu.VMEM(strips, f32),
            pltpu.VMEM(strips, f32),
            pltpu.VMEM(strips, f32),
            pltpu.VMEM((2, 3, columns // 2, 128), f32),
            pltpu.VMEM((2, 3, columns // 2, 128), f32),
            pltpu.VMEM(face, f32),
            pltpu.VMEM(face, f32),
            dma((4,)),
            dma((2, n_gy - 1)),
            dma((2, n_gy - 1)),
            dma((2, n_gy - 1)),
            dma((n_gy + 1,)),
            dma((2, 2)),
            dma((2, 2, eyd)),
            dma((2, 2)),
            dma((2, 2)),
            dma((2, n_gy - 1)),
        ],
        compiler_params=pltpu.CompilerParams(
            vmem_limit_bytes=40 * 1024 * 1024, collective_id=0, has_side_effects=True
        ),
        name="elements",
    )(sorting, counts, label, *hbm)


def yz_pass(position_ref, field_ref, far_lo_ref, far_hi_ref, ret_ref, out_ref, drag_ref, buf_ref, sem):
    _, exd, eyd, ez, _ = field_ref.shape
    at = lax.axis_index("gy")
    first = at > 0
    last = at < lax.axis_size("gy") - 1
    place = lane_iota((ez, 128)) % 64
    k = lane_iota((ez, 128)) % 8
    row = lax.broadcasted_iota(jnp.int32, (ez, 128), 0)
    up = (k == 7) & (row < ez - 1)
    down = (k == 0) & (row > 0)

    def out_copy(c, x):
        return pltpu.make_async_copy(buf_ref.at[c, x], out_ref.at[c, x], sem.at[c, x])

    def layer(index, carry):
        c, x = lax.div(index, exd), lax.rem(index, exd)
        far_lo = jnp.where(last, far_lo_ref[c, x], 0.0)
        far_hi = jnp.where(first, far_hi_ref[c, x], 0.0)
        for q in range(4):
            spot = slice(q * 128, (q + 1) * 128)
            cells = [field_ref[c, x, y, :, spot] for y in range(eyd)]
            for y in range(eyd):
                if y + 1 < eyd:
                    above = pltpu.roll(cells[y + 1], 56, 1)
                else:
                    above = pltpu.roll(far_lo, (56 - 8 * q) % 128, 1)
                if y > 0:
                    below = pltpu.roll(cells[y - 1], 72, 1)
                else:
                    below = pltpu.roll(far_hi, (72 + 8 * q) % 128, 1)
                v = cells[y] + jnp.where(place >= 56, above, 0.0) + jnp.where(place < 8, below, 0.0)
                nxt = pltpu.roll(pltpu.roll(v, ez - 1, 0), 7, 1)
                prv = pltpu.roll(pltpu.roll(v, 1, 0), 121, 1)
                buf_ref[c, x, y, :, spot] = v + jnp.where(up, nxt, 0.0) + jnp.where(down, prv, 0.0)
        out_copy(c, x).start()
        return carry

    lax.fori_loop(0, 3 * exd, layer, 0)

    def pick(index, carry):
        spots = [position_ref[index * 8 + u] for u in range(8)]
        for c in range(3):
            drag_ref[c, pl.ds(pl.multiple_of(index * 8, 8), 8), :] = rows_of([line(ret_ref, c, at) for at in spots])
        return carry

    lax.fori_loop(0, ret_ref.shape[1] // 8, pick, 0)

    def drain(index, carry):
        out_copy(lax.div(index, exd), lax.rem(index, exd)).wait()
        return carry

    lax.fori_loop(0, 3 * exd, drain, 0)


def run_yz(position, field, far_lo, far_hi, ret):
    f32 = jnp.float32
    return pl.pallas_call(
        yz_pass,
        out_shape=(jax.ShapeDtypeStruct(field.shape, f32), jax.ShapeDtypeStruct(ret.shape, f32)),
        in_specs=[pl.BlockSpec(memory_space=SMEM)] + [pl.BlockSpec(memory_space=VMEM)] * 4,
        out_specs=[pl.BlockSpec(memory_space=pl.ANY), pl.BlockSpec(memory_space=VMEM)],
        scratch_shapes=[pltpu.VMEM(field.shape, f32), pltpu.SemaphoreType.DMA(field.shape[:2])],
        compiler_params=pltpu.CompilerParams(vmem_limit_bytes=32 * 1024 * 1024),
        name="yzpass",
    )(position, field, far_lo, far_hi, ret)


def inverse_of(position):
    n = position.shape[0]
    ladder = jnp.arange(n, dtype=jnp.int32)
    return jnp.sum(jnp.where(position[None, :] == ladder[:, None], ladder[None, :], 0), axis=1)


def body(velocity, part_pos, part_vel, part_coef, counts, dest, elem):
    _, exd, eyd, ez, nodes = velocity.shape
    elems = exd * eyd * ez
    devices = lax.axis_size("gy")
    share = elems // devices
    ladder = jnp.arange(elems, dtype=jnp.int32)
    earlier = (dest[None, :] == dest[:, None]) & (ladder[None, :] < ladder[:, None])
    rank = jnp.sum(earlier.astype(jnp.int32), axis=1)
    position = dest * share + rank
    sorting = inverse_of(position)
    cells = jnp.arange(devices * 256, dtype=jnp.int32)[:, None]
    tags = jnp.where(cells == (dest * 256 + rank)[None, :], elem[None, :], 0)
    slots = jnp.where(
        cells == (dest * 256 + 128 + elem)[None, :], (lax.axis_index("gy") * share + rank)[None, :], 0
    )
    label = jnp.sum(tags + slots, axis=1).reshape(devices, 1, 256)
    field, far_lo, far_hi, ret = run_main(
        sorting, counts, label, part_pos.transpose(1, 0, 2), part_vel.transpose(1, 0, 2), part_coef,
        velocity.reshape(3, elems, nodes), (exd, eyd, ez),
    )
    source, drag_out = run_yz(position, field, far_lo, far_hi, ret)
    return (drag_out.transpose(1, 0, 2), source)


def solution(mesh):
    in_specs = (
        P(None, "gx", "gy", None, None),
        P(("gx", "gy"), None, None),
        P(("gx", "gy"), None, None),
        P(("gx", "gy"), None, None),
        P(("gx", "gy")),
        P(("gx", "gy")),
        P(("gx", "gy")),
    )
    out_specs = (P(("gx", "gy"), None, None), P(None, "gx", "gy", None, None))
    return jax.shard_map(body, mesh=mesh, in_specs=in_specs, out_specs=out_specs, check_vma=False)
```

```python
import functools
import math

import jax
import jax.numpy as jnp
from jax import lax
from jax.experimental import pallas as pl
from jax.experimental.pallas import tpu as pltpu
from jax.sharding import PartitionSpec as P

GLL = (
    -1.0,
    -0.8717401485096066,
    -0.5917001814331423,
    -0.2092992179024789,
    0.2092992179024789,
    0.5917001814331423,
    0.8717401485096066,
    1.0,
)
SHARPNESS = 8.0
WIDTH = math.sqrt(SHARPNESS * math.log2(math.e))
VMEM = pltpu.VMEM
SMEM = pltpu.SMEM
ROWS = 24


def lane_iota(shape):
    return lax.broadcasted_iota(jnp.int32, shape, len(shape) - 1)


def node_consts():
    row = lax.broadcasted_iota(jnp.int32, (8, 128), 0)

    def pick(values):
        out = jnp.full((8, 128), values[7], jnp.float32)
        for i in range(7):
            out = jnp.where(row == i, jnp.float32(values[i]), out)
        return out

    others = [pick([[GLL[m] for m in range(8) if m != i][n] for i in range(8)]) for n in range(7)]
    scales = []
    for i in range(8):
        product = 1.0
        for m in range(8):
            if m != i:
                product *= GLL[i] - GLL[m]
        scales.append(1.0 / product)
    return pick(GLL), others, pick(scales)


def lagrange(x, others, scale):
    diffs = [x - o for o in others]
    left = (diffs[0] * diffs[1]) * (diffs[2] * diffs[3])
    right = (diffs[4] * diffs[5]) * (diffs[6] * scale)
    return left * right


def gauss(x, nodes):
    gap = nodes - x
    return jnp.exp2(-(gap * gap))


def split(x):
    high = x.astype(jnp.bfloat16)
    low = (x - high.astype(jnp.float32)).astype(jnp.bfloat16)
    return high, low


def planes(a, b):
    return jnp.concatenate([a[j : j + 1] * b for j in range(8)], axis=0)


def spread_nodes(vel_ref, vs_ref, elems):
    low = lane_iota((elems, 128)) < 64
    for c in range(3):
        for q in range(4):
            x = vel_ref[c, :, q * 128 : (q + 1) * 128].astype(jnp.float32)
            turned = pltpu.roll(x, 64, 1)
            vs_ref[pl.ds(c * 8 + 2 * q, elems, stride=ROWS), :] = jnp.where(low, x, turned)
            vs_ref[pl.ds(c * 8 + 2 * q + 1, elems, stride=ROWS), :] = jnp.where(low, turned, x)


def rows_of(refs):
    return jnp.concatenate(refs, axis=0)


def project(left, both_planes):
    top, rest = split(left)
    both = jnp.concatenate([jnp.concatenate([top, top], axis=1), jnp.concatenate([rest, rest], axis=1)], axis=0)
    out = lax.dot_general(
        both, both_planes, (((1,), (1,)), ((), ())), preferred_element_type=jnp.float32
    )
    return out[: left.shape[0]] + out[left.shape[0] :]


def st_planes(s, t, nodes):
    return split(planes(gauss(s, nodes), gauss(t, nodes)))


def line(ref, c, at):
    return ref[c, pl.ds(at, 1), :]


def wide_line(ref, c, at):
    return jnp.broadcast_to(line(ref, c, at), (8, 128))


def main_kernel(
    shape, n_gx, n_gy,
    position_ref, sorting_ref, count_ref, label_ref, pos_hbm, vel_hbm, coef_hbm, velocity_hbm,
    field_ref, final_ref,
    pos_in, vel_in, coef_in, vel_ref, send_pos, send_rest, got_pos, got_rest, got_label, slot_row, tag_s, slot_s,
    vs_ref, fluid_ref, drag_ref, dep_ref, ts_ref, fs_ref,
    pos_ref, gpos_ref, out_ref, gdrag_ref, face_ref, gface_ref, lo_ref, hi_ref, ret_ref, weight_ref, plane_ref, far_lo_ref, far_hi_ref,
    in_sem, label_sem, block_sem, rest_sem, tag_sem, pos_sem, drag_sem, face_sem, y_sem, back_sem,
):
    exd, eyd, ez = shape
    elems = exd * eyd * ez
    columns = eyd * ez
    share = elems // n_gy
    half = columns // 2
    group = 16
    per = share // group
    near = n_gy // 2
    i32 = jnp.int32
    gx = lax.axis_index("gx")
    gy = lax.axis_index("gy")
    has = (gx > 0, gx < n_gx - 1)
    mesh_id = pl.DeviceIdType.MESH

    def partner(m):
        total, bit = 0, 1
        while bit < n_gy:
            total = total + lax.rem(lax.div(gy, bit) + lax.div(m, bit), 2) * bit
            bit *= 2
        return total

    pairs = ((pos_hbm, pos_in), (vel_hbm, vel_in), (coef_hbm, coef_in), (velocity_hbm, vel_ref))
    inputs = [pltpu.make_async_copy(src, dst, in_sem.at[i]) for i, (src, dst) in enumerate(pairs)]
    for copy in inputs:
        copy.start()

    def side_id(side):
        return {"gx": gx - 1 if side == 0 else gx + 1}

    def to_side(side, src, dst, sems, *at):
        return pltpu.make_async_remote_copy(
            src_ref=src, dst_ref=dst, send_sem=sems.at[(0, side) + at], recv_sem=sems.at[(1, 1 - side) + at],
            device_id=side_id(side), device_id_type=mesh_id,
        )

    def from_side(side, src, dst, sems, *at):
        return pltpu.make_async_remote_copy(
            src_ref=src, dst_ref=dst, send_sem=sems.at[(0, side) + at], recv_sem=sems.at[(1, side) + at],
            device_id=side_id(side), device_id_type=mesh_id,
        )

    barrier = pltpu.get_barrier_semaphore()
    for side in range(2):
        @pl.when(has[side])
        def _():
            pl.semaphore_signal(barrier, inc=1, device_id=side_id(side), device_id_type=mesh_id)
    for m in range(1, n_gy):
        pl.semaphore_signal(barrier, inc=1, device_id={"gy": partner(m)}, device_id_type=mesh_id)

    def peer_copy(src, dst, sems, m):
        return pltpu.make_async_remote_copy(
            src_ref=src, dst_ref=dst, send_sem=sems.at[0, m - 1], recv_sem=sems.at[1, m - 1],
            device_id={"gy": partner(m)}, device_id_type=mesh_id,
        )

    def part(index):
        return pl.ds(pl.multiple_of(index * share, 8), share)

    def label_copy(m):
        return peer_copy(label_ref.at[partner(m)], got_label.at[gy], label_sem, m)

    def pos_copy(m):
        return peer_copy(send_pos.at[:, part(partner(m))], got_pos.at[:, part(gy)], block_sem, m)

    def rest_copy(m):
        return peer_copy(send_rest.at[:, part(partner(m))], got_rest.at[:, part(gy)], rest_sem, m)

    def back_copy(m):
        return peer_copy(drag_ref.at[:, part(partner(m))], ret_ref.at[:, part(gy)], back_sem, m)

    def tag_copy(index, m):
        return pltpu.make_async_copy(got_label.at[index], tag_s.at[index], tag_sem.at[m])

    lane = lane_iota((1, 128))

    def pack_pos(dst, index):
        def some(i, carry):
            start = pl.multiple_of(index * share + i * 8, 8)
            spots = [sorting_ref[start + u] for u in range(8)]
            for c in range(3):
                dst[c, pl.ds(start, 8), :] = rows_of([line(pos_in, c, b) for b in spots])
            return carry

        lax.fori_loop(0, share // 8, some, 0)

    def pack_rest(dst, index):
        def some(i, carry):
            start = pl.multiple_of(index * share + i * 8, 8)
            spots = [sorting_ref[start + u] for u in range(8)]
            for c in range(3):
                dst[c, pl.ds(start, 8), :] = rows_of([line(vel_in, c, b) for b in spots])
            dst[3, pl.ds(start, 8), :] = rows_of(
                [jnp.where(lane < count_ref[b], coef_in[b, 0:1, :], 0.0) for b in spots]
            )
            dst[4, pl.ds(start, 8), :] = rows_of([coef_in[b, 1:2, :] for b in spots])
            return carry

        lax.fori_loop(0, share // 8, some, 0)

    for side in range(2):
        @pl.when(jnp.logical_not(has[side]))
        def _():
            gpos_ref[side] = jnp.zeros(gpos_ref.shape[1:], jnp.float32)
            gdrag_ref[side] = jnp.zeros(gdrag_ref.shape[1:], jnp.float32)

    got_label[gy] = label_ref[gy]
    tag_copy(gy, 0).start()
    order = tuple(range(near, n_gy)) + tuple(range(1, near))
    inputs[0].wait()
    for m in order[: n_gy - near]:
        pack_pos(send_pos, partner(m))
    pl.semaphore_wait(barrier, n_gy - 1 + has[0].astype(i32) + has[1].astype(i32))
    for m in order:
        label_copy(m).start()
    for m in order[: n_gy - near]:
        pos_copy(m).start()
    inputs[1].wait()
    inputs[2].wait()
    for m in order[: n_gy - near]:
        pack_rest(send_rest, partner(m))
    for m in order[n_gy - near :]:
        pack_pos(send_pos, partner(m))
        pos_copy(m).start()
        pack_rest(send_rest, partner(m))
        rest_copy(m).start()
    pack_pos(got_pos, gy)
    pack_rest(got_rest, gy)
    inputs[3].wait()
    spread_nodes(vel_ref, vs_ref, elems)
    consts = node_consts()
    nodes, others, scale = consts
    nodes = nodes * WIDTH
    tag_copy(gy, 0).wait()

    def slot_of(e):
        return slot_s[0, e]

    def collect(dst, src, start, count):
        def some(i, carry):
            for side in range(2):
                at = pl.multiple_of(start + i * 8, 8)
                spots = [slot_of(side * columns + at + u) for u in range(8)]
                for c in range(3):
                    dst[side, c, pl.ds(at, 8), :] = rows_of([line(src, c, b) for b in spots])
            return carry

        lax.fori_loop(0, count // 8, some, 0)

    slot_copy = pltpu.make_async_copy(slot_row, slot_s, tag_sem.at[n_gy])

    def interpolate(index, carry):
        @pl.when(index == per)
        def _():
            for m in order:
                label_copy(m).wait()
            total = got_label[0]
            for other in range(1, n_gy):
                total = total + got_label[other]
            slot_row[...] = total[:, 128:]
            slot_copy.start()
            for m in order:
                tag_copy(partner(m), m).start()
            for m in range(near, n_gy):
                pos_copy(m).wait_send()
                rest_copy(m).start()
            slot_copy.wait()
            for m in order:
                tag_copy(partner(m), m).wait()

        for m in range(1, near):
            @pl.when(index == m * per)
            def _():
                pos_copy(m).wait()

        @pl.when(index == near * per)
        def _():
            for m in range(near, n_gy):
                pos_copy(m).wait_recv()
            collect(pos_ref, got_pos, 0, columns)
            for side in range(2):
                @pl.when(has[side])
                def _():
                    to_side(side, pos_ref.at[side], gpos_ref.at[1 - side], pos_sem).start()

        source = partner(lax.div(index, per))
        first = lax.rem(index, per) * group
        for batch in range(group // 8):
            fluid = [[], [], []]
            for u in range(8):
                i = first + batch * 8 + u
                slot = source * share + i
                e = tag_s[source, 0, i]
                r, s, t = (wide_line(got_pos, d, slot) for d in range(3))
                basis_r = lagrange(r, others, scale)
                high, low = split(planes(lagrange(s, others, scale), lagrange(t, others, scale)))
                partial = jnp.dot(
                    vs_ref[pl.ds(e * ROWS, ROWS), :].astype(jnp.bfloat16),
                    jnp.concatenate([high, low], axis=0),
                    preferred_element_type=jnp.float32,
                )
                for c in range(3):
                    fluid[c].append(jnp.sum(partial[c * 8 : c * 8 + 8] * basis_r, axis=0, keepdims=True))
            at = pl.multiple_of(source * share + first + batch * 8, 8)
            for c in range(3):
                fluid_ref[c, pl.ds(at, 8), :] = rows_of(fluid[c])
        return carry

    lax.fori_loop(0, elems // group, interpolate, 0)

    def forces(start, count):
        def some(i, carry):
            m = lax.div(start + i * 8, share)
            at = pl.ds(pl.multiple_of(partner(m) * share + lax.rem(start + i * 8, share), 8), 8)
            rel = [fluid_ref[c, at, :] - got_rest[c, at, :] for c in range(3)]
            speed = jnp.sqrt(rel[0] * rel[0] + rel[1] * rel[1] + rel[2] * rel[2])
            power = jnp.exp(0.687 * jnp.log(got_rest[4, at, :] * speed))
            factor = got_rest[3, at, :] * (1.0 + 0.15 * power)
            for c in range(3):
                drag_ref[c, at, :] = factor * rel[c]
            return carry

        lax.fori_loop(0, count // 8, some, 0)

    def strip(k):
        return lax.rem(k * (eyd - 1), eyd)

    def drag_copy(make, side, y):
        at = pl.ds(pl.multiple_of(y * ez, 8), ez)
        return make(side, out_ref.at[side, :, at], gdrag_ref.at[1 - side, :, at], drag_sem, y)

    def strip_start(k):
        for side in range(2):
            @pl.when(has[side])
            def _():
                drag_copy(to_side, side, k * (eyd - 1) % eyd).start()

    def strip_sent(k):
        for side in range(2):
            @pl.when(has[side])
            def _():
                drag_copy(to_side, side, k * (eyd - 1) % eyd).wait_send()

    def deposit(index, carry):
        @pl.when(index == 0)
        def _():
            for m in range(1, near):
                rest_copy(m).wait()
            forces(0, near * share)

        @pl.when(index == near * per)
        def _():
            for m in range(near, n_gy):
                rest_copy(m).wait()
            forces(near * share, elems - near * share)
            collect(out_ref, drag_ref, 0, columns)
            for k in range(eyd):
                strip_start(k)
            for m in order:
                back_copy(m).start()
            ret_ref[:, part(gy), :] = drag_ref[:, part(gy), :]

        source = partner(lax.div(index, per))
        first = lax.rem(index, per) * group
        for u in range(group):
            i = first + u
            slot = source * share + i
            layer = jnp.full((8, 128), tag_s[source, 0, i], i32)
            shift = jnp.where(layer < columns, -2.0 * WIDTH, 2.0 * WIDTH)
            r, s, t = (wide_line(got_pos, d, slot) * WIDTH for d in range(3))
            weights = (gauss(r, nodes), gauss(r + shift, nodes))
            force = [-line(drag_ref, c, slot) for c in range(3)]
            left = jnp.concatenate([f * w for w in weights for f in force], axis=0)
            out = project(left, jnp.concatenate(st_planes(s, t, nodes), axis=1))
            dep_ref[pl.ds(pl.multiple_of(slot * 2 * ROWS, 8), 2 * ROWS), 0:64] = out
        return carry

    lax.fori_loop(0, elems // group, deposit, 0)

    def gather(i, carry):
        for side in range(exd):
            spots = []
            for u in range(8):
                col = i * 8 + u
                mine = slot_of(side * columns + col) * (2 * ROWS)
                other = slot_of((1 - side) * columns + col) * (2 * ROWS) + ROWS
                e = side * columns + col
                ts_ref[pl.ds(pl.multiple_of(e * ROWS, 8), ROWS), :] = (
                    dep_ref[pl.ds(mine, ROWS), :] + dep_ref[pl.ds(other, ROWS), :]
                )
                spots.append(mine)
            node = 0 if side == 0 else 7
            for c in range(3):
                fs_ref[side, c, pl.ds(pl.multiple_of(i * 8, 8), 8), :] = rows_of(
                    [dep_ref[pl.ds(at + c * 8 + node, 1), :] for at in spots]
                )
        return carry

    lax.fori_loop(0, columns // 8, gather, 0)

    base = (0, elems - columns)
    low_h = lane_iota((half, 128)) < 64
    for side in range(2):
        node = 0 if side == 0 else 7
        for c in range(3):
            one = ts_ref[pl.ds(base[side] * ROWS + c * 8 + node, half, stride=ROWS), :]
            two = ts_ref[pl.ds((base[side] + half) * ROWS + c * 8 + node, half, stride=ROWS), :]
            face_ref[side, c] = jnp.where(low_h, one, pltpu.roll(two, 64, 1))
        @pl.when(has[side])
        def _():
            to_side(side, face_ref.at[side], gface_ref.at[1 - side], face_sem).start()

    for side in range(2):
        @pl.when(has[side])
        def _():
            from_side(side, pos_ref.at[side], gpos_ref.at[side], pos_sem).wait()

    def prepare(k, carry):
        for side in range(2):
            for g in range(8):
                col = k * 8 + g
                r, s, t = (jnp.broadcast_to(gpos_ref[side, d, pl.ds(col, 1), :], (8, 128)) * WIDTH for d in range(3))
                weight_ref[side, col] = gauss(r + (-2.0 if side == 0 else 2.0) * WIDTH, nodes)
                plane_ref[side, col] = jnp.concatenate(st_planes(s, t, nodes), axis=1)
        return carry

    lax.fori_loop(0, columns // 8, prepare, 0)

    def pick(i, carry):
        at = pl.multiple_of(i * 8, 8)
        spots = [position_ref[at + u] for u in range(8)]
        for c in range(3):
            final_ref[c, pl.ds(at, 8), :] = rows_of([line(ret_ref, c, spot) for spot in spots])
        return carry

    for m in order:
        back_copy(m).wait()
    lax.fori_loop(0, elems // 8, pick, 0)

    def ghost(k, carry):
        y = strip(k)
        at = pl.ds(pl.multiple_of(y * ez, 8), ez)
        for side in range(2):
            @pl.when(has[side])
            def _():
                from_side(side, out_ref.at[side, :, at], gdrag_ref.at[side, :, at], drag_sem, y).wait_recv()
        sums = []
        for side in range(2):
            for g in range(ez):
                col = y * ez + g
                weight = weight_ref[side, col]
                left = jnp.concatenate([(-gdrag_ref[side, c, pl.ds(col, 1), :]) * weight for c in range(3)], axis=0)
                add = project(left, plane_ref[side, col])
                spot = pl.ds(pl.multiple_of((base[side] + col) * ROWS, 8), ROWS)
                sums.append((spot, ts_ref[spot, 0:64] + add))
        for spot, value in sums:
            ts_ref[spot, 0:64] = value
        return carry

    lax.fori_loop(0, eyd, ghost, 0)

    for side in range(2):
        @pl.when(has[side])
        def _():
            from_side(side, face_ref.at[side], gface_ref.at[side], face_sem).wait()

    low = lane_iota((ez, 128)) < 64
    spot64 = lane_iota((ez, 128)) % 64
    depth = lax.broadcasted_iota(jnp.int32, (ez, 128), 0)
    up = (spot64 % 8 == 7) & (depth < ez - 1)
    down = (spot64 % 8 == 0) & (depth > 0)
    lo_copy = pltpu.make_async_remote_copy(
        src_ref=lo_ref, dst_ref=far_lo_ref, send_sem=y_sem.at[0, 0], recv_sem=y_sem.at[1, 0],
        device_id={"gy": gy - 1}, device_id_type=mesh_id,
    )
    hi_copy = pltpu.make_async_remote_copy(
        src_ref=hi_ref, dst_ref=far_hi_ref, send_sem=y_sem.at[0, 1], recv_sem=y_sem.at[1, 1],
        device_id={"gy": gy + 1}, device_id_type=mesh_id,
    )

    def assemble(k, carry):
        y = strip(k)
        upper = y >= eyd // 2

        def lanes(c, x, q):
            start = (x * columns + y * ez) * ROWS + c * 8 + 2 * q
            even = ts_ref[pl.ds(start, ez, stride=ROWS), :]
            odd = ts_ref[pl.ds(start + 1, ez, stride=ROWS), :]
            return jnp.where(low, even, pltpu.roll(odd, 64, 1))

        def far(c, side):
            came = gface_ref[side, c, pl.ds(pl.multiple_of(lax.rem(y, eyd // 2) * ez, 8), ez), :]
            turned = pltpu.roll(came, 64, 1)
            came = jnp.where(low != upper, came, turned)
            mine = fs_ref[side, c, pl.ds(pl.multiple_of(y * ez, 8), ez), :]
            mine = jnp.where(low, mine, pltpu.roll(mine, 64, 1))
            return jnp.where(has[side], came + mine, 0.0)

        edges = []
        for c in range(3):
            grid = [[lanes(c, x, q) for q in range(4)] for x in range(exd)]
            for x in range(exd):
                above = pltpu.roll(grid[x + 1][0], 64, 1) if x + 1 < exd else far(c, 1)
                below = pltpu.roll(grid[x - 1][3], 64, 1) if x > 0 else far(c, 0)
                done = list(grid[x])
                done[3] = done[3] + jnp.where(low, 0.0, above)
                done[0] = done[0] + jnp.where(low, below, 0.0)
                for q in range(4):
                    nxt = pltpu.roll(pltpu.roll(done[q], ez - 1, 0), 7, 1)
                    prv = pltpu.roll(pltpu.roll(done[q], 1, 0), 121, 1)
                    done[q] = done[q] + jnp.where(up, nxt, 0.0) + jnp.where(down, prv, 0.0)
                for q in range(4):
                    field_ref[c, x, y, :, q * 128 : (q + 1) * 128] = done[q]

                edges.append((c, x, done))

        @pl.when(k == 0)
        def _():
            for c, x, done in edges:
                face = jnp.where(spot64 < 8, done[0], 0.0)
                for q in range(1, 4):
                    face = face + pltpu.roll(jnp.where(spot64 < 8, done[q], 0.0), 8 * q, 1)
                lo_ref[c, x] = face

            @pl.when(gy > 0)
            def _():
                lo_copy.start()

        @pl.when(k == 1)
        def _():
            for c, x, done in edges:
                face = jnp.where(spot64 >= 56, done[0], 0.0)
                for q in range(1, 4):
                    face = face + pltpu.roll(jnp.where(spot64 >= 56, done[q], 0.0), 128 - 8 * q, 1)
                hi_ref[c, x] = face

            @pl.when(gy < n_gy - 1)
            def _():
                hi_copy.start()

        return carry

    lax.fori_loop(0, eyd, assemble, 0)

    def across(c, carry):
        for x in range(exd):
            for q in range(4):
                spot = slice(q * 128, (q + 1) * 128)
                cells = [field_ref[c, x, y, :, spot] for y in range(eyd)]
                for y in range(eyd):
                    v = cells[y]
                    if y + 1 < eyd:
                        v = v + jnp.where(spot64 >= 56, pltpu.roll(cells[y + 1], 56, 1), 0.0)
                    if y > 0:
                        v = v + jnp.where(spot64 < 8, pltpu.roll(cells[y - 1], 72, 1), 0.0)
                    field_ref[c, x, y, :, spot] = v
        return carry

    lax.fori_loop(0, 3, across, 0)
    for k in range(eyd):
        strip_sent(k)

    def edge(far_ref, y, keep, turn):
        for c in range(3):
            for x in range(exd):
                far_edge = far_ref[c, x]
                for q in range(4):
                    spot = slice(q * 128, (q + 1) * 128)
                    add = jnp.where(keep, pltpu.roll(far_edge, turn(q) % 128, 1), 0.0)
                    field_ref[c, x, y, :, spot] = field_ref[c, x, y, :, spot] + add

    @pl.when(gy > 0)
    def _():
        hi_copy.wait_recv()
        edge(far_hi_ref, 0, spot64 < 8, lambda q: 72 + 8 * q)
        lo_copy.wait_send()

    @pl.when(gy < n_gy - 1)
    def _():
        lo_copy.wait_recv()
        edge(far_lo_ref, eyd - 1, spot64 >= 56, lambda q: 56 - 8 * q)
        hi_copy.wait_send()


def run_main(position, sorting, counts, label, pos, vel, coef, velocity, shape):
    exd, eyd, ez = shape
    elems = exd * eyd * ez
    columns = eyd * ez
    n_gx, n_gy = lax.axis_size("gx"), lax.axis_size("gy")
    f32, i32 = jnp.float32, jnp.int32
    dma = pltpu.SemaphoreType.DMA
    face = (3, exd, ez, 128)
    strips = (2, 3, columns, 128)
    hbm = [pltpu.with_memory_space_constraint(x, pltpu.HBM) for x in (pos, vel, coef, velocity)]
    return pl.pallas_call(
        functools.partial(main_kernel, shape, n_gx, n_gy),
        out_shape=(
            jax.ShapeDtypeStruct((3, exd, eyd, ez, 512), f32),
            jax.ShapeDtypeStruct((3, elems, 128), f32),
        ),
        in_specs=[pl.BlockSpec(memory_space=SMEM)] * 3
        + [pl.BlockSpec(memory_space=VMEM)]
        + [pl.BlockSpec(memory_space=pltpu.HBM)] * 4,
        out_specs=[pl.BlockSpec(memory_space=VMEM)] * 2,
        scratch_shapes=[
            pltpu.VMEM(pos.shape, f32),
            pltpu.VMEM(vel.shape, f32),
            pltpu.VMEM(coef.shape, f32),
            pltpu.VMEM(velocity.shape, velocity.dtype),
            pltpu.VMEM((3, elems, 128), f32),
            pltpu.VMEM((5, elems, 128), f32),
            pltpu.VMEM((3, elems, 128), f32),
            pltpu.VMEM((5, elems, 128), f32),
            pltpu.VMEM(label.shape, i32),
            pltpu.VMEM((1, 128), i32),
            pltpu.SMEM(label.shape, i32),
            pltpu.SMEM((1, 128), i32),
            pltpu.VMEM((elems * ROWS, 128), f32),
            pltpu.VMEM((3, elems, 128), f32),
            pltpu.VMEM((3, elems, 128), f32),
            pltpu.VMEM((elems * 2 * ROWS, 128), f32),
            pltpu.VMEM((elems * ROWS, 128), f32),
            pltpu.VMEM(strips, f32),
            pltpu.VMEM(strips, f32),
            pltpu.VMEM(strips, f32),
            pltpu.VMEM(strips, f32),
            pltpu.VMEM(strips, f32),
            pltpu.VMEM((2, 3, columns // 2, 128), f32),
            pltpu.VMEM((2, 3, columns // 2, 128), f32),
            pltpu.VMEM(face, f32),
            pltpu.VMEM(face, f32),
            pltpu.VMEM((3, elems, 128), f32),
            pltpu.VMEM((2, columns, 8, 128), f32),
            pltpu.VMEM((2, columns, 64, 256), jnp.bfloat16),
            pltpu.VMEM(face, f32),
            pltpu.VMEM(face, f32),
            dma((4,)),
            dma((2, n_gy - 1)),
            dma((2, n_gy - 1)),
            dma((2, n_gy - 1)),
            dma((n_gy + 1,)),
            dma((2, 2)),
            dma((2, 2, eyd)),
            dma((2, 2)),
            dma((2, 2)),
            dma((2, n_gy - 1)),
        ],
        compiler_params=pltpu.CompilerParams(
            vmem_limit_bytes=40 * 1024 * 1024, collective_id=0, has_side_effects=True
        ),
        name="elements",
    )(position, sorting, counts, label, *hbm)


def store_pass(field_ref, final_ref, out_ref, drag_ref, sem):
    copies = [pltpu.make_async_copy(field_ref.at[c], out_ref.at[c], sem.at[c]) for c in range(3)]
    copies.append(pltpu.make_async_copy(final_ref, drag_ref, sem.at[3]))
    for copy in copies:
        copy.start()
    for copy in copies:
        copy.wait()


def run_store(field, final):
    f32 = jnp.float32
    return pl.pallas_call(
        store_pass,
        out_shape=(jax.ShapeDtypeStruct(field.shape, f32), jax.ShapeDtypeStruct(final.shape, f32)),
        in_specs=[pl.BlockSpec(memory_space=VMEM)] * 2,
        out_specs=[pl.BlockSpec(memory_space=pl.ANY)] * 2,
        scratch_shapes=[pltpu.SemaphoreType.DMA((4,))],
        compiler_params=pltpu.CompilerParams(vmem_limit_bytes=32 * 1024 * 1024),
        name="store",
    )(field, final)


def inverse_of(position):
    n = position.shape[0]
    ladder = jnp.arange(n, dtype=jnp.int32)
    return jnp.sum(jnp.where(position[None, :] == ladder[:, None], ladder[None, :], 0), axis=1)


def body(velocity, part_pos, part_vel, part_coef, counts, dest, elem):
    _, exd, eyd, ez, nodes = velocity.shape
    elems = exd * eyd * ez
    devices = lax.axis_size("gy")
    share = elems // devices
    ladder = jnp.arange(elems, dtype=jnp.int32)
    earlier = (dest[None, :] == dest[:, None]) & (ladder[None, :] < ladder[:, None])
    rank = jnp.sum(earlier.astype(jnp.int32), axis=1)
    position = dest * share + rank
    sorting = inverse_of(position)
    cells = jnp.arange(devices * 256, dtype=jnp.int32)[:, None]
    tags = jnp.where(cells == (dest * 256 + rank)[None, :], elem[None, :], 0)
    slots = jnp.where(
        cells == (dest * 256 + 128 + elem)[None, :], (lax.axis_index("gy") * share + rank)[None, :], 0
    )
    label = jnp.sum(tags + slots, axis=1).reshape(devices, 1, 256)
    field, final = run_main(
        position, sorting, counts, label, part_pos.transpose(1, 0, 2), part_vel.transpose(1, 0, 2), part_coef,
        velocity.reshape(3, elems, nodes), (exd, eyd, ez),
    )
    source, drag_out = run_store(field, final)
    return (drag_out.transpose(1, 0, 2), source)


def solution(mesh):
    in_specs = (
        P(None, "gx", "gy", None, None),
        P(("gx", "gy"), None, None),
        P(("gx", "gy"), None, None),
        P(("gx", "gy"), None, None),
        P(("gx", "gy")),
        P(("gx", "gy")),
        P(("gx", "gy")),
    )
    out_specs = (P(("gx", "gy"), None, None), P(None, "gx", "gy", None, None))
    return jax.shard_map(body, mesh=mesh, in_specs=in_specs, out_specs=out_specs, check_vma=False)
```

```python
import functools
import math

import jax
import jax.numpy as jnp
from jax import lax
from jax.experimental import pallas as pl
from jax.experimental.pallas import tpu as pltpu
from jax.sharding import PartitionSpec as P

GLL = (
    -1.0,
    -0.8717401485096066,
    -0.5917001814331423,
    -0.2092992179024789,
    0.2092992179024789,
    0.5917001814331423,
    0.8717401485096066,
    1.0,
)
SHARPNESS = 8.0
WIDTH = math.sqrt(SHARPNESS * math.log2(math.e))
VMEM = pltpu.VMEM
SMEM = pltpu.SMEM
ROWS = 24


def lane_iota(shape):
    return lax.broadcasted_iota(jnp.int32, shape, len(shape) - 1)


def node_consts():
    row = lax.broadcasted_iota(jnp.int32, (8, 128), 0)

    def pick(values):
        out = jnp.full((8, 128), values[7], jnp.float32)
        for i in range(7):
            out = jnp.where(row == i, jnp.float32(values[i]), out)
        return out

    others = [pick([[GLL[m] for m in range(8) if m != i][n] for i in range(8)]) for n in range(7)]
    scales = []
    for i in range(8):
        product = 1.0
        for m in range(8):
            if m != i:
                product *= GLL[i] - GLL[m]
        scales.append(1.0 / product)
    return pick(GLL), others, pick(scales)


def lagrange(x, others, scale):
    diffs = [x - o for o in others]
    left = (diffs[0] * diffs[1]) * (diffs[2] * diffs[3])
    right = (diffs[4] * diffs[5]) * (diffs[6] * scale)
    return left * right


def gauss(x, nodes):
    gap = nodes - x
    return jnp.exp2(-(gap * gap))


def split(x):
    high = x.astype(jnp.bfloat16)
    low = (x - high.astype(jnp.float32)).astype(jnp.bfloat16)
    return high, low


def planes(a, b):
    return jnp.concatenate([a[j : j + 1] * b for j in range(8)], axis=0)


def spread_nodes(vel_ref, vs_ref, elems):
    low = lane_iota((elems, 128)) < 64
    for c in range(3):
        for q in range(4):
            x = vel_ref[c, :, q * 128 : (q + 1) * 128].astype(jnp.float32)
            turned = pltpu.roll(x, 64, 1)
            vs_ref[pl.ds(c * 8 + 2 * q, elems, stride=ROWS), :] = jnp.where(low, x, turned)
            vs_ref[pl.ds(c * 8 + 2 * q + 1, elems, stride=ROWS), :] = jnp.where(low, turned, x)


def rows_of(refs):
    return jnp.concatenate(refs, axis=0)


def project(left, both_planes):
    top, rest = split(left)
    both = jnp.concatenate([jnp.concatenate([top, top], axis=1), jnp.concatenate([rest, rest], axis=1)], axis=0)
    out = lax.dot_general(
        both, both_planes, (((1,), (1,)), ((), ())), preferred_element_type=jnp.float32
    )
    return out[: left.shape[0]] + out[left.shape[0] :]


def st_planes(s, t, nodes):
    return split(planes(gauss(s, nodes), gauss(t, nodes)))


def line(ref, c, at):
    return ref[c, pl.ds(at, 1), :]


def wide_line(ref, c, at):
    return jnp.broadcast_to(line(ref, c, at), (8, 128))


def main_kernel(
    shape, n_gx, n_gy,
    dest_hbm, elem_hbm, count_hbm, pos_hbm, vel_hbm, coef_hbm, velocity_hbm,
    field_ref, final_ref,
    dest_in, elem_in, count_in, pos_in, vel_in, coef_in, vel_ref, label_ref, place_row, position_ref, send_pos, send_rest, got_pos, got_rest, got_label, slot_row, tag_s, slot_s,
    vs_ref, fluid_ref, drag_ref, dep_ref, ts_ref, fs_ref,
    pos_ref, gpos_ref, out_ref, gdrag_ref, face_ref, gface_ref, lo_ref, hi_ref, ret_ref, weight_ref, plane_ref, far_lo_ref, far_hi_ref,
    in_sem, label_sem, block_sem, rest_sem, tag_sem, pos_sem, drag_sem, face_sem, y_sem, back_sem,
):
    exd, eyd, ez = shape
    elems = exd * eyd * ez
    columns = eyd * ez
    share = elems // n_gy
    half = columns // 2
    group = 16
    per = share // group
    near = n_gy // 2
    i32 = jnp.int32
    gx = lax.axis_index("gx")
    gy = lax.axis_index("gy")
    has = (gx > 0, gx < n_gx - 1)
    mesh_id = pl.DeviceIdType.MESH

    def partner(m):
        total, bit = 0, 1
        while bit < n_gy:
            total = total + lax.rem(lax.div(gy, bit) + lax.div(m, bit), 2) * bit
            bit *= 2
        return total

    pairs = (
        (dest_hbm, dest_in), (elem_hbm, elem_in), (count_hbm, count_in),
        (pos_hbm, pos_in), (vel_hbm, vel_in), (coef_hbm, coef_in), (velocity_hbm, vel_ref),
    )
    inputs = [pltpu.make_async_copy(src, dst, in_sem.at[i]) for i, (src, dst) in enumerate(pairs)]
    for copy in inputs:
        copy.start()

    def side_id(side):
        return {"gx": gx - 1 if side == 0 else gx + 1}

    def to_side(side, src, dst, sems, *at):
        return pltpu.make_async_remote_copy(
            src_ref=src, dst_ref=dst, send_sem=sems.at[(0, side) + at], recv_sem=sems.at[(1, 1 - side) + at],
            device_id=side_id(side), device_id_type=mesh_id,
        )

    def from_side(side, src, dst, sems, *at):
        return pltpu.make_async_remote_copy(
            src_ref=src, dst_ref=dst, send_sem=sems.at[(0, side) + at], recv_sem=sems.at[(1, side) + at],
            device_id=side_id(side), device_id_type=mesh_id,
        )

    barrier = pltpu.get_barrier_semaphore()
    for side in range(2):
        @pl.when(has[side])
        def _():
            pl.semaphore_signal(barrier, inc=1, device_id=side_id(side), device_id_type=mesh_id)
    for m in range(1, n_gy):
        pl.semaphore_signal(barrier, inc=1, device_id={"gy": partner(m)}, device_id_type=mesh_id)

    def peer_copy(src, dst, sems, m):
        return pltpu.make_async_remote_copy(
            src_ref=src, dst_ref=dst, send_sem=sems.at[0, m - 1], recv_sem=sems.at[1, m - 1],
            device_id={"gy": partner(m)}, device_id_type=mesh_id,
        )

    def part(index):
        return pl.ds(pl.multiple_of(index * share, 8), share)

    def label_copy(m):
        return peer_copy(label_ref.at[partner(m)], got_label.at[gy], label_sem, m)

    def pos_copy(m):
        return peer_copy(send_pos.at[:, part(partner(m))], got_pos.at[:, part(gy)], block_sem, m)

    def rest_copy(m):
        return peer_copy(send_rest.at[:, part(partner(m))], got_rest.at[:, part(gy)], rest_sem, m)

    def back_copy(m):
        return peer_copy(drag_ref.at[:, part(partner(m))], ret_ref.at[:, part(gy)], back_sem, m)

    def tag_copy(index, m):
        return pltpu.make_async_copy(got_label.at[index], tag_s.at[index], tag_sem.at[m])

    for side in range(2):
        @pl.when(jnp.logical_not(has[side]))
        def _():
            gpos_ref[side] = jnp.zeros(gpos_ref.shape[1:], jnp.float32)
            gdrag_ref[side] = jnp.zeros(gdrag_ref.shape[1:], jnp.float32)

    f32, bf16 = jnp.float32, jnp.bfloat16
    across_lanes = (((1,), (1,)), ((), ()))
    height = lax.broadcasted_iota(i32, (elems, elems), 0)
    for copy in inputs[:3]:
        copy.wait()
    dest_row, elem_row = dest_in[...], elem_in[...]
    square = (elems, elems)
    wide = lane_iota(square)

    def turned(x):
        return jnp.broadcast_to(x, square).T

    def summed(x):
        while x.shape[0] > 8:
            x = x[: x.shape[0] // 2] + x[x.shape[0] // 2 :]
        for step in (4, 2, 1):
            x = x + pltpu.roll(x, step, 0)
        return x[0:1]

    dest_col, elem_col = turned(dest_row), turned(elem_row)
    rank = summed(jnp.where((dest_col == dest_row) & (height < wide), 1, 0))
    place = dest_row * share + rank
    place_row[...] = place
    place_copy = pltpu.make_async_copy(place_row, position_ref, tag_sem.at[n_gy + 1])
    place_copy.start()
    chosen = (place == height).astype(bf16)
    place_col = turned(place)
    tags = summed(jnp.where(place_col == wide, elem_col, 0))
    slot_col = place_col + (gy - dest_col) * share
    slot_col = jnp.where(elem_col == wide, slot_col, 0)
    for d in range(n_gy):
        label_ref[d] = jnp.concatenate([tags, summed(jnp.where(dest_col == d, slot_col, 0))], axis=1)

    def in_order(x):
        top = x.astype(bf16)
        left = x - top.astype(f32)
        middle = left.astype(bf16)
        bottom = (left - middle.astype(f32)).astype(bf16)
        return (
            jnp.dot(chosen, top, preferred_element_type=f32)
            + jnp.dot(chosen, middle, preferred_element_type=f32)
            + jnp.dot(chosen, bottom, preferred_element_type=f32)
        )

    order = tuple(range(near, n_gy)) + tuple(range(1, near))
    inputs[3].wait()
    both = in_order(jnp.concatenate([pos_in[0], pos_in[1]], axis=1))
    send_pos[0] = both[:, :128]
    send_pos[1] = both[:, 128:]
    send_pos[2] = in_order(pos_in[2])
    pl.semaphore_wait(barrier, n_gy - 1 + has[0].astype(i32) + has[1].astype(i32))
    for m in order:
        label_copy(m).start()
    for m in order:
        pos_copy(m).start()
    got_label[gy] = label_ref[gy]
    tag_copy(gy, 0).start()
    got_pos[:, part(gy), :] = send_pos[:, part(gy), :]
    inputs[4].wait()
    inputs[5].wait()
    both = in_order(jnp.concatenate([vel_in[0], vel_in[1]], axis=1))
    send_rest[0] = both[:, :128]
    send_rest[1] = both[:, 128:]
    both = in_order(jnp.concatenate([vel_in[2], coef_in[pl.ds(0, elems, stride=2), :]], axis=1))
    live = lax.dot_general(
        chosen, jnp.broadcast_to(count_in[...].astype(f32), (128, elems)).astype(bf16), across_lanes,
        preferred_element_type=f32,
    )
    send_rest[2] = both[:, :128]
    send_rest[3] = jnp.where(lane_iota((elems, 128)).astype(f32) < live, both[:, 128:], 0.0)
    send_rest[4] = in_order(coef_in[pl.ds(1, elems, stride=2), :])
    for m in range(1, near):
        rest_copy(m).start()
    got_rest[:, part(gy), :] = send_rest[:, part(gy), :]
    inputs[6].wait()
    spread_nodes(vel_ref, vs_ref, elems)
    consts = node_consts()
    nodes, others, scale = consts
    nodes = nodes * WIDTH
    tag_copy(gy, 0).wait()

    def within(i):
        return jnp.minimum(jnp.maximum(i, 0), elems - 1)

    def slot_of(e):
        return within(slot_s[0, e])

    def collect(dst, src, start, count):
        def some(i, carry):
            for side in range(2):
                at = pl.multiple_of(start + i * 8, 8)
                spots = [slot_of(side * columns + at + u) for u in range(8)]
                for c in range(3):
                    dst[side, c, pl.ds(at, 8), :] = rows_of([line(src, c, b) for b in spots])
            return carry

        lax.fori_loop(0, count // 8, some, 0)

    slot_copy = pltpu.make_async_copy(slot_row, slot_s, tag_sem.at[n_gy])

    def interpolate(index, carry):
        @pl.when(index == per)
        def _():
            for m in order:
                label_copy(m).wait()
            total = got_label[0]
            for other in range(1, n_gy):
                total = total + got_label[other]
            slot_row[...] = total[:, 128:]
            slot_copy.start()
            for m in order:
                tag_copy(partner(m), m).start()
            for m in range(near, n_gy):
                pos_copy(m).wait_send()
                rest_copy(m).start()
            slot_copy.wait()
            for m in order:
                tag_copy(partner(m), m).wait()

        for m in range(1, near):
            @pl.when(index == m * per)
            def _():
                pos_copy(m).wait()

        @pl.when(index == near * per)
        def _():
            for m in range(near, n_gy):
                pos_copy(m).wait_recv()
            collect(pos_ref, got_pos, 0, columns)
            for side in range(2):
                @pl.when(has[side])
                def _():
                    to_side(side, pos_ref.at[side], gpos_ref.at[1 - side], pos_sem).start()

        source = partner(lax.div(index, per))
        first = lax.rem(index, per) * group
        for batch in range(group // 8):
            fluid = [[], [], []]
            for u in range(8):
                i = first + batch * 8 + u
                slot = source * share + i
                e = within(tag_s[source, 0, gy * share + i])
                r, s, t = (wide_line(got_pos, d, slot) for d in range(3))
                basis_r = lagrange(r, others, scale)
                high, low = split(planes(lagrange(s, others, scale), lagrange(t, others, scale)))
                partial = jnp.dot(
                    vs_ref[pl.ds(e * ROWS, ROWS), :].astype(jnp.bfloat16),
                    jnp.concatenate([high, low], axis=0),
                    preferred_element_type=jnp.float32,
                )
                for c in range(3):
                    fluid[c].append(jnp.sum(partial[c * 8 : c * 8 + 8] * basis_r, axis=0, keepdims=True))
            at = pl.multiple_of(source * share + first + batch * 8, 8)
            for c in range(3):
                fluid_ref[c, pl.ds(at, 8), :] = rows_of(fluid[c])
        return carry

    lax.fori_loop(0, elems // group, interpolate, 0)

    def forces(start, count):
        def some(i, carry):
            m = lax.div(start + i * 8, share)
            at = pl.ds(pl.multiple_of(partner(m) * share + lax.rem(start + i * 8, share), 8), 8)
            rel = [fluid_ref[c, at, :] - got_rest[c, at, :] for c in range(3)]
            speed = jnp.sqrt(rel[0] * rel[0] + rel[1] * rel[1] + rel[2] * rel[2])
            power = jnp.exp(0.687 * jnp.log(got_rest[4, at, :] * speed))
            factor = got_rest[3, at, :] * (1.0 + 0.15 * power)
            for c in range(3):
                drag_ref[c, at, :] = factor * rel[c]
            return carry

        lax.fori_loop(0, count // 8, some, 0)

    def strip(k):
        return lax.rem(k * (eyd - 1), eyd)

    def drag_copy(make, side, y):
        at = pl.ds(pl.multiple_of(y * ez, 8), ez)
        return make(side, out_ref.at[side, :, at], gdrag_ref.at[1 - side, :, at], drag_sem, y)

    def strip_start(k):
        for side in range(2):
            @pl.when(has[side])
            def _():
                drag_copy(to_side, side, k * (eyd - 1) % eyd).start()

    def strip_sent(k):
        for side in range(2):
            @pl.when(has[side])
            def _():
                drag_copy(to_side, side, k * (eyd - 1) % eyd).wait_send()

    def deposit(index, carry):
        @pl.when(index == 0)
        def _():
            for m in range(1, near):
                rest_copy(m).wait()
            forces(0, near * share)

        @pl.when(index == near * per)
        def _():
            for m in range(near, n_gy):
                rest_copy(m).wait()
            forces(near * share, elems - near * share)
            collect(out_ref, drag_ref, 0, columns)
            for k in range(eyd):
                strip_start(k)
            for m in order:
                back_copy(m).start()
            ret_ref[:, part(gy), :] = drag_ref[:, part(gy), :]

        source = partner(lax.div(index, per))
        first = lax.rem(index, per) * group
        for u in range(group):
            i = first + u
            slot = source * share + i
            layer = jnp.full((8, 128), tag_s[source, 0, gy * share + i], i32)
            shift = jnp.where(layer < columns, -2.0 * WIDTH, 2.0 * WIDTH)
            r, s, t = (wide_line(got_pos, d, slot) * WIDTH for d in range(3))
            weights = (gauss(r, nodes), gauss(r + shift, nodes))
            force = [-line(drag_ref, c, slot) for c in range(3)]
            left = jnp.concatenate([f * w for w in weights for f in force], axis=0)
            out = project(left, jnp.concatenate(st_planes(s, t, nodes), axis=1))
            dep_ref[pl.ds(pl.multiple_of(slot * 2 * ROWS, 8), 2 * ROWS), 0:64] = out
        return carry

    lax.fori_loop(0, elems // group, deposit, 0)

    def gather(i, carry):
        for side in range(exd):
            spots = []
            for u in range(8):
                col = i * 8 + u
                mine = slot_of(side * columns + col) * (2 * ROWS)
                other = slot_of((1 - side) * columns + col) * (2 * ROWS) + ROWS
                e = side * columns + col
                ts_ref[pl.ds(pl.multiple_of(e * ROWS, 8), ROWS), :] = (
                    dep_ref[pl.ds(mine, ROWS), :] + dep_ref[pl.ds(other, ROWS), :]
                )
                spots.append(mine)
            node = 0 if side == 0 else 7
            for c in range(3):
                fs_ref[side, c, pl.ds(pl.multiple_of(i * 8, 8), 8), :] = rows_of(
                    [dep_ref[pl.ds(at + c * 8 + node, 1), :] for at in spots]
                )
        return carry

    lax.fori_loop(0, columns // 8, gather, 0)

    base = (0, elems - columns)
    low_h = lane_iota((half, 128)) < 64
    for side in range(2):
        node = 0 if side == 0 else 7
        for c in range(3):
            one = ts_ref[pl.ds(base[side] * ROWS + c * 8 + node, half, stride=ROWS), :]
            two = ts_ref[pl.ds((base[side] + half) * ROWS + c * 8 + node, half, stride=ROWS), :]
            face_ref[side, c] = jnp.where(low_h, one, pltpu.roll(two, 64, 1))
        @pl.when(has[side])
        def _():
            to_side(side, face_ref.at[side], gface_ref.at[1 - side], face_sem).start()

    for side in range(2):
        @pl.when(has[side])
        def _():
            from_side(side, pos_ref.at[side], gpos_ref.at[side], pos_sem).wait()

    def prepare(k, carry):
        for side in range(2):
            for g in range(8):
                col = k * 8 + g
                r, s, t = (jnp.broadcast_to(gpos_ref[side, d, pl.ds(col, 1), :], (8, 128)) * WIDTH for d in range(3))
                weight_ref[side, col] = gauss(r + (-2.0 if side == 0 else 2.0) * WIDTH, nodes)
                plane_ref[side, col] = jnp.concatenate(st_planes(s, t, nodes), axis=1)
        return carry

    lax.fori_loop(0, columns // 8, prepare, 0)

    def pick(i, carry):
        at = pl.multiple_of(i * 8, 8)
        spots = [within(position_ref[0, at + u]) for u in range(8)]
        for c in range(3):
            final_ref[c, pl.ds(at, 8), :] = rows_of([line(ret_ref, c, spot) for spot in spots])
        return carry

    place_copy.wait()
    for m in order:
        back_copy(m).wait()
    lax.fori_loop(0, elems // 8, pick, 0)

    def ghost(k, carry):
        y = strip(k)
        at = pl.ds(pl.multiple_of(y * ez, 8), ez)
        for side in range(2):
            @pl.when(has[side])
            def _():
                from_side(side, out_ref.at[side, :, at], gdrag_ref.at[side, :, at], drag_sem, y).wait_recv()
        sums = []
        for side in range(2):
            for g in range(ez):
                col = y * ez + g
                weight = weight_ref[side, col]
                left = jnp.concatenate([(-gdrag_ref[side, c, pl.ds(col, 1), :]) * weight for c in range(3)], axis=0)
                add = project(left, plane_ref[side, col])
                spot = pl.ds(pl.multiple_of((base[side] + col) * ROWS, 8), ROWS)
                sums.append((spot, ts_ref[spot, 0:64] + add))
        for spot, value in sums:
            ts_ref[spot, 0:64] = value
        return carry

    lax.fori_loop(0, eyd, ghost, 0)

    for side in range(2):
        @pl.when(has[side])
        def _():
            from_side(side, face_ref.at[side], gface_ref.at[side], face_sem).wait()

    low = lane_iota((ez, 128)) < 64
    spot64 = lane_iota((ez, 128)) % 64
    depth = lax.broadcasted_iota(jnp.int32, (ez, 128), 0)
    up = (spot64 % 8 == 7) & (depth < ez - 1)
    down = (spot64 % 8 == 0) & (depth > 0)
    lo_copy = pltpu.make_async_remote_copy(
        src_ref=lo_ref, dst_ref=far_lo_ref, send_sem=y_sem.at[0, 0], recv_sem=y_sem.at[1, 0],
        device_id={"gy": gy - 1}, device_id_type=mesh_id,
    )
    hi_copy = pltpu.make_async_remote_copy(
        src_ref=hi_ref, dst_ref=far_hi_ref, send_sem=y_sem.at[0, 1], recv_sem=y_sem.at[1, 1],
        device_id={"gy": gy + 1}, device_id_type=mesh_id,
    )

    def assemble(k, carry):
        y = strip(k)
        upper = y >= eyd // 2

        def lanes(c, x, q):
            start = (x * columns + y * ez) * ROWS + c * 8 + 2 * q
            even = ts_ref[pl.ds(start, ez, stride=ROWS), :]
            odd = ts_ref[pl.ds(start + 1, ez, stride=ROWS), :]
            return jnp.where(low, even, pltpu.roll(odd, 64, 1))

        def far(c, side):
            came = gface_ref[side, c, pl.ds(pl.multiple_of(lax.rem(y, eyd // 2) * ez, 8), ez), :]
            turned = pltpu.roll(came, 64, 1)
            came = jnp.where(low != upper, came, turned)
            mine = fs_ref[side, c, pl.ds(pl.multiple_of(y * ez, 8), ez), :]
            mine = jnp.where(low, mine, pltpu.roll(mine, 64, 1))
            return jnp.where(has[side], came + mine, 0.0)

        edges = []
        for c in range(3):
            grid = [[lanes(c, x, q) for q in range(4)] for x in range(exd)]
            for x in range(exd):
                above = pltpu.roll(grid[x + 1][0], 64, 1) if x + 1 < exd else far(c, 1)
                below = pltpu.roll(grid[x - 1][3], 64, 1) if x > 0 else far(c, 0)
                done = list(grid[x])
                done[3] = done[3] + jnp.where(low, 0.0, above)
                done[0] = done[0] + jnp.where(low, below, 0.0)
                for q in range(4):
                    nxt = pltpu.roll(pltpu.roll(done[q], ez - 1, 0), 7, 1)
                    prv = pltpu.roll(pltpu.roll(done[q], 1, 0), 121, 1)
                    done[q] = done[q] + jnp.where(up, nxt, 0.0) + jnp.where(down, prv, 0.0)
                for q in range(4):
                    field_ref[c, x, y, :, q * 128 : (q + 1) * 128] = done[q]

                edges.append((c, x, done))

        @pl.when(k == 0)
        def _():
            for c, x, done in edges:
                face = jnp.where(spot64 < 8, done[0], 0.0)
                for q in range(1, 4):
                    face = face + pltpu.roll(jnp.where(spot64 < 8, done[q], 0.0), 8 * q, 1)
                lo_ref[c, x] = face

            @pl.when(gy > 0)
            def _():
                lo_copy.start()

        @pl.when(k == 1)
        def _():
            for c, x, done in edges:
                face = jnp.where(spot64 >= 56, done[0], 0.0)
                for q in range(1, 4):
                    face = face + pltpu.roll(jnp.where(spot64 >= 56, done[q], 0.0), 128 - 8 * q, 1)
                hi_ref[c, x] = face

            @pl.when(gy < n_gy - 1)
            def _():
                hi_copy.start()

        return carry

    lax.fori_loop(0, eyd, assemble, 0)

    def across(c, carry):
        for x in range(exd):
            for q in range(4):
                spot = slice(q * 128, (q + 1) * 128)
                cells = [field_ref[c, x, y, :, spot] for y in range(eyd)]
                for y in range(eyd):
                    v = cells[y]
                    if y + 1 < eyd:
                        v = v + jnp.where(spot64 >= 56, pltpu.roll(cells[y + 1], 56, 1), 0.0)
                    if y > 0:
                        v = v + jnp.where(spot64 < 8, pltpu.roll(cells[y - 1], 72, 1), 0.0)
                    field_ref[c, x, y, :, spot] = v
        return carry

    lax.fori_loop(0, 3, across, 0)
    for k in range(eyd):
        strip_sent(k)

    def edge(far_ref, y, keep, turn):
        for c in range(3):
            for x in range(exd):
                far_edge = far_ref[c, x]
                for q in range(4):
                    spot = slice(q * 128, (q + 1) * 128)
                    add = jnp.where(keep, pltpu.roll(far_edge, turn(q) % 128, 1), 0.0)
                    field_ref[c, x, y, :, spot] = field_ref[c, x, y, :, spot] + add

    @pl.when(gy > 0)
    def _():
        hi_copy.wait_recv()
        edge(far_hi_ref, 0, spot64 < 8, lambda q: 72 + 8 * q)
        lo_copy.wait_send()

    @pl.when(gy < n_gy - 1)
    def _():
        lo_copy.wait_recv()
        edge(far_lo_ref, eyd - 1, spot64 >= 56, lambda q: 56 - 8 * q)
        hi_copy.wait_send()


def run_main(arrays, shape):
    exd, eyd, ez = shape
    elems = exd * eyd * ez
    columns = eyd * ez
    n_gx, n_gy = lax.axis_size("gx"), lax.axis_size("gy")
    f32, i32 = jnp.float32, jnp.int32
    dma = pltpu.SemaphoreType.DMA
    face = (3, exd, ez, 128)
    label = (n_gy, 1, 2 * elems)
    strips = (2, 3, columns, 128)
    hbm = [pltpu.with_memory_space_constraint(x, pltpu.HBM) for x in arrays]
    return pl.pallas_call(
        functools.partial(main_kernel, shape, n_gx, n_gy),
        out_shape=(
            jax.ShapeDtypeStruct((3, exd, eyd, ez, 512), f32),
            jax.ShapeDtypeStruct((3, elems, 128), f32),
        ),
        in_specs=[pl.BlockSpec(memory_space=pltpu.HBM)] * len(hbm),
        out_specs=[pl.BlockSpec(memory_space=VMEM)] * 2,
        scratch_shapes=[
            *(pltpu.VMEM(x.shape, x.dtype) for x in arrays),
            pltpu.VMEM(label, i32),
            pltpu.VMEM((1, elems), i32),
            pltpu.SMEM((1, elems), i32),
            pltpu.VMEM((3, elems, 128), f32),
            pltpu.VMEM((5, elems, 128), f32),
            pltpu.VMEM((3, elems, 128), f32),
            pltpu.VMEM((5, elems, 128), f32),
            pltpu.VMEM(label, i32),
            pltpu.VMEM((1, 128), i32),
            pltpu.SMEM(label, i32),
            pltpu.SMEM((1, 128), i32),
            pltpu.VMEM((elems * ROWS, 128), f32),
            pltpu.VMEM((3, elems, 128), f32),
            pltpu.VMEM((3, elems, 128), f32),
            pltpu.VMEM((elems * 2 * ROWS, 128), f32),
            pltpu.VMEM((elems * ROWS, 128), f32),
            pltpu.VMEM(strips, f32),
            pltpu.VMEM(strips, f32),
            pltpu.VMEM(strips, f32),
            pltpu.VMEM(strips, f32),
            pltpu.VMEM(strips, f32),
            pltpu.VMEM((2, 3, columns // 2, 128), f32),
            pltpu.VMEM((2, 3, columns // 2, 128), f32),
            pltpu.VMEM(face, f32),
            pltpu.VMEM(face, f32),
            pltpu.VMEM((3, elems, 128), f32),
            pltpu.VMEM((2, columns, 8, 128), f32),
            pltpu.VMEM((2, columns, 64, 256), jnp.bfloat16),
            pltpu.VMEM(face, f32),
            pltpu.VMEM(face, f32),
            dma((len(hbm),)),
            dma((2, n_gy - 1)),
            dma((2, n_gy - 1)),
            dma((2, n_gy - 1)),
            dma((n_gy + 2,)),
            dma((2, 2)),
            dma((2, 2, eyd)),
            dma((2, 2)),
            dma((2, 2)),
            dma((2, n_gy - 1)),
        ],
        compiler_params=pltpu.CompilerParams(
            vmem_limit_bytes=40 * 1024 * 1024, collective_id=0, has_side_effects=True
        ),
        name="elements",
    )(*hbm)


def store_pass(field_ref, final_ref, out_ref, drag_ref, sem):
    copies = [pltpu.make_async_copy(field_ref.at[c], out_ref.at[c], sem.at[c]) for c in range(3)]
    copies.append(pltpu.make_async_copy(final_ref, drag_ref, sem.at[3]))
    for copy in copies:
        copy.start()
    for copy in copies:
        copy.wait()


def run_store(field, final):
    f32 = jnp.float32
    return pl.pallas_call(
        store_pass,
        out_shape=(jax.ShapeDtypeStruct(field.shape, f32), jax.ShapeDtypeStruct(final.shape, f32)),
        in_specs=[pl.BlockSpec(memory_space=VMEM)] * 2,
        out_specs=[pl.BlockSpec(memory_space=pl.ANY)] * 2,
        scratch_shapes=[pltpu.SemaphoreType.DMA((4,))],
        compiler_params=pltpu.CompilerParams(vmem_limit_bytes=32 * 1024 * 1024),
        name="store",
    )(field, final)


def body(velocity, part_pos, part_vel, part_coef, counts, dest, elem):
    _, exd, eyd, ez, nodes = velocity.shape
    elems = exd * eyd * ez
    arrays = (
        dest.reshape(1, elems), elem.reshape(1, elems), counts.reshape(1, elems),
        part_pos.transpose(1, 0, 2), part_vel.transpose(1, 0, 2), part_coef.reshape(2 * elems, 128),
        velocity.reshape(3, elems, nodes),
    )
    source, drag_out = run_store(*run_main(arrays, (exd, eyd, ez)))
    return (drag_out.transpose(1, 0, 2), source)


def solution(mesh):
    in_specs = (
        P(None, "gx", "gy", None, None),
        P(("gx", "gy"), None, None),
        P(("gx", "gy"), None, None),
        P(("gx", "gy"), None, None),
        P(("gx", "gy")),
        P(("gx", "gy")),
        P(("gx", "gy")),
    )
    out_specs = (P(("gx", "gy"), None, None), P(None, "gx", "gy", None, None))
    return jax.shard_map(body, mesh=mesh, in_specs=in_specs, out_specs=out_specs, check_vma=False)
```

```python
import functools
import math

import jax
import jax.numpy as jnp
from jax import lax
from jax.experimental import pallas as pl
from jax.experimental.pallas import tpu as pltpu
from jax.sharding import PartitionSpec as P

GLL = (
    -1.0,
    -0.8717401485096066,
    -0.5917001814331423,
    -0.2092992179024789,
    0.2092992179024789,
    0.5917001814331423,
    0.8717401485096066,
    1.0,
)
SHARPNESS = 8.0
WIDTH = math.sqrt(SHARPNESS * math.log2(math.e))
VMEM = pltpu.VMEM
SMEM = pltpu.SMEM
ROWS = 24


def lane_iota(shape):
    return lax.broadcasted_iota(jnp.int32, shape, len(shape) - 1)


def node_consts():
    row = lax.broadcasted_iota(jnp.int32, (8, 128), 0)

    def pick(values):
        out = jnp.full((8, 128), values[7], jnp.float32)
        for i in range(7):
            out = jnp.where(row == i, jnp.float32(values[i]), out)
        return out

    others = [pick([[GLL[m] for m in range(8) if m != i][n] for i in range(8)]) for n in range(7)]
    scales = []
    for i in range(8):
        product = 1.0
        for m in range(8):
            if m != i:
                product *= GLL[i] - GLL[m]
        scales.append(1.0 / product)
    return pick(GLL), others, pick(scales)


def lagrange(x, others, scale):
    diffs = [x - o for o in others]
    left = (diffs[0] * diffs[1]) * (diffs[2] * diffs[3])
    right = (diffs[4] * diffs[5]) * (diffs[6] * scale)
    return left * right


def gauss(x, nodes):
    gap = nodes - x
    return jnp.exp2(-(gap * gap))


def split(x):
    high = x.astype(jnp.bfloat16)
    low = (x - high.astype(jnp.float32)).astype(jnp.bfloat16)
    return high, low


def planes(a, b):
    return jnp.concatenate([a[j : j + 1] * b for j in range(8)], axis=0)


def spread_nodes(vel_ref, vs_ref, elems):
    low = lane_iota((elems, 128)) < 64
    for c in range(3):
        for q in range(4):
            x = vel_ref[c, :, q * 128 : (q + 1) * 128].astype(jnp.float32)
            turned = pltpu.roll(x, 64, 1)
            vs_ref[pl.ds(c * 8 + 2 * q, elems, stride=ROWS), :] = jnp.where(low, x, turned)
            vs_ref[pl.ds(c * 8 + 2 * q + 1, elems, stride=ROWS), :] = jnp.where(low, turned, x)


def rows_of(refs):
    return jnp.concatenate(refs, axis=0)


def project(left, both_planes):
    top, rest = split(left)
    both = jnp.concatenate([jnp.concatenate([top, top], axis=1), jnp.concatenate([rest, rest], axis=1)], axis=0)
    out = lax.dot_general(
        both, both_planes, (((1,), (1,)), ((), ())), preferred_element_type=jnp.float32
    )
    return out[: left.shape[0]] + out[left.shape[0] :]


def st_planes(s, t, nodes):
    return split(planes(gauss(s, nodes), gauss(t, nodes)))


def line(ref, c, at):
    return ref[c, pl.ds(at, 1), :]


def wide_line(ref, c, at):
    return jnp.broadcast_to(line(ref, c, at), (8, 128))


def main_kernel(
    shape, n_gx, n_gy,
    dest_hbm, elem_hbm, count_hbm, pos_hbm, vel_hbm, coef_hbm, velocity_hbm,
    field_ref, final_ref,
    dest_in, elem_in, count_in, pos_in, vel_in, coef_in, vel_ref, label_ref, place_row, position_ref, send_pos, send_rest, got_pos, got_rest, got_label, slot_row, tag_s, slot_s,
    vs_ref, fluid_ref, drag_ref, dep_ref, ts_ref, fs_ref,
    pos_ref, gpos_ref, out_ref, gdrag_ref, face_ref, gface_ref, lo_ref, hi_ref, ret_ref, weight_ref, plane_ref, far_lo_ref, far_hi_ref,
    in_sem, label_sem, block_sem, rest_sem, tag_sem, pos_sem, drag_sem, face_sem, y_sem, back_sem,
):
    exd, eyd, ez = shape
    elems = exd * eyd * ez
    columns = eyd * ez
    share = elems // n_gy
    group = 16
    per = share // group
    near = n_gy // 2
    i32 = jnp.int32
    gx = lax.axis_index("gx")
    gy = lax.axis_index("gy")
    has = (gx > 0, gx < n_gx - 1)
    mesh_id = pl.DeviceIdType.MESH

    def partner(m):
        total, bit = 0, 1
        while bit < n_gy:
            total = total + lax.rem(lax.div(gy, bit) + lax.div(m, bit), 2) * bit
            bit *= 2
        return total

    pairs = (
        (dest_hbm, dest_in), (elem_hbm, elem_in), (count_hbm, count_in),
        (pos_hbm, pos_in), (vel_hbm, vel_in), (coef_hbm, coef_in), (velocity_hbm, vel_ref),
    )
    inputs = [pltpu.make_async_copy(src, dst, in_sem.at[i]) for i, (src, dst) in enumerate(pairs)]
    for copy in inputs:
        copy.start()

    def side_id(side):
        return {"gx": gx - 1 if side == 0 else gx + 1}

    def to_side(side, src, dst, sems, *at):
        return pltpu.make_async_remote_copy(
            src_ref=src, dst_ref=dst, send_sem=sems.at[(0, side) + at], recv_sem=sems.at[(1, 1 - side) + at],
            device_id=side_id(side), device_id_type=mesh_id,
        )

    def from_side(side, src, dst, sems, *at):
        return pltpu.make_async_remote_copy(
            src_ref=src, dst_ref=dst, send_sem=sems.at[(0, side) + at], recv_sem=sems.at[(1, side) + at],
            device_id=side_id(side), device_id_type=mesh_id,
        )

    barrier = pltpu.get_barrier_semaphore()
    for side in range(2):
        @pl.when(has[side])
        def _():
            pl.semaphore_signal(barrier, inc=1, device_id=side_id(side), device_id_type=mesh_id)
    for m in range(1, n_gy):
        pl.semaphore_signal(barrier, inc=1, device_id={"gy": partner(m)}, device_id_type=mesh_id)

    def peer_copy(src, dst, sems, m):
        return pltpu.make_async_remote_copy(
            src_ref=src, dst_ref=dst, send_sem=sems.at[0, m - 1], recv_sem=sems.at[1, m - 1],
            device_id={"gy": partner(m)}, device_id_type=mesh_id,
        )

    def part(index):
        return pl.ds(pl.multiple_of(index * share, 8), share)

    def label_copy(m):
        return peer_copy(label_ref.at[partner(m)], got_label.at[gy], label_sem, m)

    def pos_copy(m):
        return peer_copy(send_pos.at[:, part(partner(m))], got_pos.at[:, part(gy)], block_sem, m)

    def rest_copy(m):
        return peer_copy(send_rest.at[:, part(partner(m))], got_rest.at[:, part(gy)], rest_sem, m)

    def back_copy(m):
        return peer_copy(drag_ref.at[:, part(partner(m))], ret_ref.at[:, part(gy)], back_sem, m)

    def tag_copy(index, m):
        return pltpu.make_async_copy(got_label.at[index], tag_s.at[index], tag_sem.at[m])

    for side in range(2):
        @pl.when(jnp.logical_not(has[side]))
        def _():
            gpos_ref[side] = jnp.zeros(gpos_ref.shape[1:], jnp.float32)
            gdrag_ref[side] = jnp.zeros(gdrag_ref.shape[1:], jnp.float32)

    f32, bf16 = jnp.float32, jnp.bfloat16
    across_lanes = (((1,), (1,)), ((), ()))
    height = lax.broadcasted_iota(i32, (elems, elems), 0)
    for copy in inputs[:3]:
        copy.wait()
    dest_row, elem_row = dest_in[...], elem_in[...]
    square = (elems, elems)
    wide = lane_iota(square)

    def turned(x):
        return jnp.broadcast_to(x, square).T

    def summed(x):
        while x.shape[0] > 8:
            x = x[: x.shape[0] // 2] + x[x.shape[0] // 2 :]
        for step in (4, 2, 1):
            x = x + pltpu.roll(x, step, 0)
        return x[0:1]

    dest_col, elem_col = turned(dest_row), turned(elem_row)
    rank = summed(jnp.where((dest_col == dest_row) & (height < wide), 1, 0))
    place = dest_row * share + rank
    place_row[...] = place
    place_copy = pltpu.make_async_copy(place_row, position_ref, tag_sem.at[n_gy + 1])
    place_copy.start()
    chosen = (place == height).astype(bf16)
    place_col = turned(place)
    tags = summed(jnp.where(place_col == wide, elem_col, 0))
    slot_col = place_col + (gy - dest_col) * share
    slot_col = jnp.where(elem_col == wide, slot_col, 0)
    for d in range(n_gy):
        label_ref[d] = jnp.concatenate([tags, summed(jnp.where(dest_col == d, slot_col, 0))], axis=1)

    def picked(chosen, x):
        top = x.astype(bf16)
        left = x - top.astype(f32)
        middle = left.astype(bf16)
        bottom = (left - middle.astype(f32)).astype(bf16)
        return (
            jnp.dot(chosen, top, preferred_element_type=f32)
            + jnp.dot(chosen, middle, preferred_element_type=f32)
            + jnp.dot(chosen, bottom, preferred_element_type=f32)
        )

    order = tuple(range(near, n_gy)) + tuple(range(1, near))
    inputs[3].wait()
    both = picked(chosen, jnp.concatenate([pos_in[0], pos_in[1]], axis=1))
    send_pos[0] = both[:, :128]
    send_pos[1] = both[:, 128:]
    send_pos[2] = picked(chosen, pos_in[2])
    pl.semaphore_wait(barrier, n_gy - 1 + has[0].astype(i32) + has[1].astype(i32))
    for m in order:
        label_copy(m).start()
    for m in order:
        pos_copy(m).start()
    got_label[gy] = label_ref[gy]
    tag_copy(gy, 0).start()
    got_pos[:, part(gy), :] = send_pos[:, part(gy), :]
    inputs[4].wait()
    inputs[5].wait()
    both = picked(chosen, jnp.concatenate([vel_in[0], vel_in[1]], axis=1))
    send_rest[0] = both[:, :128]
    send_rest[1] = both[:, 128:]
    both = picked(chosen, jnp.concatenate([vel_in[2], coef_in[pl.ds(0, elems, stride=2), :]], axis=1))
    live = lax.dot_general(
        chosen, jnp.broadcast_to(count_in[...].astype(f32), (128, elems)).astype(bf16), across_lanes,
        preferred_element_type=f32,
    )
    send_rest[2] = both[:, :128]
    send_rest[3] = jnp.where(lane_iota((elems, 128)).astype(f32) < live, both[:, 128:], 0.0)
    send_rest[4] = picked(chosen, coef_in[pl.ds(1, elems, stride=2), :])
    for m in range(1, near):
        rest_copy(m).start()
    got_rest[:, part(gy), :] = send_rest[:, part(gy), :]
    inputs[6].wait()
    spread_nodes(vel_ref, vs_ref, elems)
    consts = node_consts()
    nodes, others, scale = consts
    nodes = nodes * WIDTH
    tag_copy(gy, 0).wait()

    def within(i):
        return jnp.minimum(jnp.maximum(i, 0), elems - 1)

    base = (0, elems - columns)

    def slot_of(e):
        return within(slot_s[0, e])

    def collect(dst, src, start, count):
        def some(i, carry):
            for side in range(2):
                at = pl.multiple_of(start + i * 8, 8)
                spots = [slot_of(side * columns + at + u) for u in range(8)]
                for c in range(3):
                    dst[side, c, pl.ds(at, 8), :] = rows_of([line(src, c, b) for b in spots])
            return carry

        lax.fori_loop(0, count // 8, some, 0)

    slot_copy = pltpu.make_async_copy(slot_row, slot_s, tag_sem.at[n_gy])

    def forces(start, count):
        def some(i, carry):
            m = lax.div(start + i * 8, share)
            at = pl.ds(pl.multiple_of(partner(m) * share + lax.rem(start + i * 8, share), 8), 8)
            rel = [fluid_ref[c, at, :] - got_rest[c, at, :] for c in range(3)]
            speed = jnp.sqrt(rel[0] * rel[0] + rel[1] * rel[1] + rel[2] * rel[2])
            power = jnp.exp(0.687 * jnp.log(got_rest[4, at, :] * speed))
            factor = got_rest[3, at, :] * (1.0 + 0.15 * power)
            for c in range(3):
                drag_ref[c, at, :] = factor * rel[c]
            return carry

        lax.fori_loop(0, count // 8, some, 0)

    def deposit_step(index, carry):
        source = partner(lax.div(index, per))
        first = lax.rem(index, per) * group
        for u in range(group):
            i = first + u
            slot = source * share + i
            layer = jnp.full((8, 128), tag_s[source, 0, gy * share + i], i32)
            shift = jnp.where(layer < columns, -2.0 * WIDTH, 2.0 * WIDTH)
            r, s, t = (wide_line(got_pos, d, slot) * WIDTH for d in range(3))
            weights = (gauss(r, nodes), gauss(r + shift, nodes))
            force = [-line(drag_ref, c, slot) for c in range(3)]
            left = jnp.concatenate([f * w for w in weights for f in force], axis=0)
            out = project(left, jnp.concatenate(st_planes(s, t, nodes), axis=1))
            dep_ref[pl.ds(pl.multiple_of(slot * 2 * ROWS, 8), 2 * ROWS), 0:64] = out
        return carry

    def interpolate(index, carry):
        @pl.when(index == per)
        def _():
            forces(0, share)
            lax.fori_loop(0, per, deposit_step, 0)
            for m in range(near, n_gy):
                pos_copy(m).wait_send()
                rest_copy(m).start()
            for m in order:
                label_copy(m).wait()
            total = got_label[0]
            for other in range(1, n_gy):
                total = total + got_label[other]
            slot_row[...] = total[:, elems:]
            slot_copy.start()
            for m in order:
                tag_copy(partner(m), m).start()
            wanted = (turned(total[:, elems:]) == wide).astype(bf16)
            for m in range(1, near):
                pos_copy(m).wait()
            for m in range(near, n_gy):
                pos_copy(m).wait_recv()
            for c in range(3):
                held = picked(wanted, got_pos[c])
                for side in range(2):
                    pos_ref[side, c] = held[base[side] : base[side] + columns]
            for side in range(2):
                @pl.when(has[side])
                def _():
                    to_side(side, pos_ref.at[side], gpos_ref.at[1 - side], pos_sem).start()
            slot_copy.wait()
            for m in order:
                tag_copy(partner(m), m).wait()

        source = partner(lax.div(index, per))
        first = lax.rem(index, per) * group
        for batch in range(group // 8):
            fluid = [[], [], []]
            for u in range(8):
                i = first + batch * 8 + u
                slot = source * share + i
                e = within(tag_s[source, 0, gy * share + i])
                r, s, t = (wide_line(got_pos, d, slot) for d in range(3))
                basis_r = lagrange(r, others, scale)
                high, low = split(planes(lagrange(s, others, scale), lagrange(t, others, scale)))
                partial = jnp.dot(
                    vs_ref[pl.ds(e * ROWS, ROWS), :].astype(jnp.bfloat16),
                    jnp.concatenate([high, low], axis=0),
                    preferred_element_type=jnp.float32,
                )
                for c in range(3):
                    fluid[c].append(jnp.sum(partial[c * 8 : c * 8 + 8] * basis_r, axis=0, keepdims=True))
            at = pl.multiple_of(source * share + first + batch * 8, 8)
            for c in range(3):
                fluid_ref[c, pl.ds(at, 8), :] = rows_of(fluid[c])
        return carry

    lax.fori_loop(0, elems // group, interpolate, 0)

    def strip(k):
        odd = lax.rem(k, 2)
        return odd * (eyd - 1) + (1 - 2 * odd) * lax.div(k, 2)

    def drag_copy(make, side, y):
        at = pl.ds(pl.multiple_of(y * ez, 8), ez)
        return make(side, out_ref.at[side, :, at], gdrag_ref.at[1 - side, :, at], drag_sem, y)

    def strip_start(k):
        for side in range(2):
            @pl.when(has[side])
            def _():
                drag_copy(to_side, side, strip(k)).start()

    def strip_sent(k):
        for side in range(2):
            @pl.when(has[side])
            def _():
                drag_copy(to_side, side, strip(k)).wait_send()

    def deposit(index, carry):
        @pl.when(index == per)
        def _():
            for m in range(1, near):
                rest_copy(m).wait()
            forces(share, (near - 1) * share)

        @pl.when(index == near * per)
        def _():
            for m in range(near, n_gy):
                rest_copy(m).wait()
            forces(near * share, elems - near * share)
            collect(out_ref, drag_ref, 0, columns)
            for k in range(2):
                strip_start(k)
            for m in order:
                back_copy(m).start()
            ret_ref[:, part(gy), :] = drag_ref[:, part(gy), :]

        return deposit_step(index, carry)

    lax.fori_loop(per, elems // group, deposit, 0)

    def gather(i, carry):
        for side in range(exd):
            spots = []
            for u in range(8):
                col = i * 8 + u
                mine = slot_of(side * columns + col) * (2 * ROWS)
                other = slot_of((1 - side) * columns + col) * (2 * ROWS) + ROWS
                e = side * columns + col
                ts_ref[pl.ds(pl.multiple_of(e * ROWS, 8), ROWS), :] = (
                    dep_ref[pl.ds(mine, ROWS), :] + dep_ref[pl.ds(other, ROWS), :]
                )
                spots.append(mine)
            node = 0 if side == 0 else 7
            for c in range(3):
                fs_ref[side, c, pl.ds(pl.multiple_of(i * 8, 8), 8), :] = rows_of(
                    [dep_ref[pl.ds(at + c * 8 + node, 1), :] for at in spots]
                )
        return carry

    lax.fori_loop(0, columns // 8, gather, 0)

    low = lane_iota((ez, 128)) < 64
    pairs = eyd // 2

    def face_copy(make, side, at):
        rows = pl.ds(pl.multiple_of(at * ez, 8), ez)
        there = 1 - side if make is to_side else side
        return make(side, face_ref.at[side, :, rows], gface_ref.at[there, :, rows], face_sem, at)

    for at in range(pairs):
        for side in range(2):
            node = 0 if side == 0 else 7
            for c in range(3):
                one = ts_ref[pl.ds((base[side] + at * ez) * ROWS + c * 8 + node, ez, stride=ROWS), :]
                two = ts_ref[pl.ds((base[side] + (eyd - 1 - at) * ez) * ROWS + c * 8 + node, ez, stride=ROWS), :]
                face_ref[side, c, at * ez : (at + 1) * ez, :] = jnp.where(low, one, pltpu.roll(two, 64, 1))
    for at in range(pairs):
        for side in range(2):
            @pl.when(has[side])
            def _():
                face_copy(to_side, side, at).start()
    for k in range(2, eyd):
        strip_start(k)

    for side in range(2):
        @pl.when(has[side])
        def _():
            from_side(side, pos_ref.at[side], gpos_ref.at[side], pos_sem).wait()

    def prepare(k, carry):
        for side in range(2):
            for g in range(8):
                col = k * 8 + g
                r, s, t = (jnp.broadcast_to(gpos_ref[side, d, pl.ds(col, 1), :], (8, 128)) * WIDTH for d in range(3))
                weight_ref[side, col] = gauss(r + (-2.0 if side == 0 else 2.0) * WIDTH, nodes)
                plane_ref[side, col] = jnp.concatenate(st_planes(s, t, nodes), axis=1)
        return carry

    lax.fori_loop(0, columns // 8, prepare, 0)

    def pick(i, carry):
        at = pl.multiple_of(i * 8, 8)
        spots = [within(position_ref[0, at + u]) for u in range(8)]
        for c in range(3):
            final_ref[c, pl.ds(at, 8), :] = rows_of([line(ret_ref, c, spot) for spot in spots])
        return carry


    def ghost(k, carry):
        y = strip(k)
        at = pl.ds(pl.multiple_of(y * ez, 8), ez)
        for side in range(2):
            @pl.when(has[side])
            def _():
                from_side(side, out_ref.at[side, :, at], gdrag_ref.at[side, :, at], drag_sem, y).wait_recv()
        sums = []
        for side in range(2):
            for g in range(ez):
                col = y * ez + g
                weight = weight_ref[side, col]
                left = jnp.concatenate([(-gdrag_ref[side, c, pl.ds(col, 1), :]) * weight for c in range(3)], axis=0)
                add = project(left, plane_ref[side, col])
                spot = pl.ds(pl.multiple_of((base[side] + col) * ROWS, 8), ROWS)
                sums.append((spot, ts_ref[spot, 0:64] + add))
        for spot, value in sums:
            ts_ref[spot, 0:64] = value
        return carry

    spot64 = lane_iota((ez, 128)) % 64
    depth = lax.broadcasted_iota(jnp.int32, (ez, 128), 0)
    up = (spot64 % 8 == 7) & (depth < ez - 1)
    down = (spot64 % 8 == 0) & (depth > 0)
    lo_copy = pltpu.make_async_remote_copy(
        src_ref=lo_ref, dst_ref=far_lo_ref, send_sem=y_sem.at[0, 0], recv_sem=y_sem.at[1, 0],
        device_id={"gy": gy - 1}, device_id_type=mesh_id,
    )
    hi_copy = pltpu.make_async_remote_copy(
        src_ref=hi_ref, dst_ref=far_hi_ref, send_sem=y_sem.at[0, 1], recv_sem=y_sem.at[1, 1],
        device_id={"gy": gy + 1}, device_id_type=mesh_id,
    )

    def through(v):
        nxt = pltpu.roll(pltpu.roll(v, ez - 1, 0), 7, 1)
        prv = pltpu.roll(pltpu.roll(v, 1, 0), 121, 1)
        return v + jnp.where(up, nxt, 0.0) + jnp.where(down, prv, 0.0)

    def lanes(c, x, y, q):
        start = (x * columns + y * ez) * ROWS + c * 8 + 2 * q
        even = ts_ref[pl.ds(start, ez, stride=ROWS), :]
        odd = ts_ref[pl.ds(start + 1, ez, stride=ROWS), :]
        return jnp.where(low, even, pltpu.roll(odd, 64, 1))

    def far(c, side, y, at, upper):
        came = gface_ref[side, c, pl.ds(pl.multiple_of(at * ez, 8), ez), :]
        turn = pltpu.roll(came, 64, 1)
        came = jnp.where(low != upper, came, turn)
        mine = fs_ref[side, c, pl.ds(pl.multiple_of(y * ez, 8), ez), :]
        mine = jnp.where(low, mine, pltpu.roll(mine, 64, 1))
        return jnp.where(has[side] & (low if side == 0 else jnp.logical_not(low)), came + mine, 0.0)

    def assembled(k):
        y = strip(k)
        out = []
        for c in range(3):
            grid = [[lanes(c, x, y, q) for q in range(4)] for x in range(exd)]
            for x in range(exd):
                done = list(grid[x])
                if x + 1 < exd:
                    done[3] = done[3] + jnp.where(low, 0.0, pltpu.roll(grid[x + 1][0], 64, 1))
                else:
                    done[3] = done[3] + far(c, 1, y, lax.div(k, 2), lax.rem(k, 2) == 1)
                if x > 0:
                    done[0] = done[0] + jnp.where(low, pltpu.roll(grid[x - 1][3], 64, 1), 0.0)
                else:
                    done[0] = done[0] + far(c, 0, y, lax.div(k, 2), lax.rem(k, 2) == 1)
                done = [through(v) for v in done]
                for q in range(4):
                    field_ref[c, x, y, :, q * 128 : (q + 1) * 128] = done[q]
                out.append((c, x, done))
        return out

    def outer(k, carry):
        edges = assembled(k)

        @pl.when(k == 0)
        def _():
            for c, x, done in edges:
                face = jnp.where(spot64 < 8, done[0], 0.0)
                for q in range(1, 4):
                    face = face + pltpu.roll(jnp.where(spot64 < 8, done[q], 0.0), 8 * q, 1)
                lo_ref[c, x] = face

            @pl.when(gy > 0)
            def _():
                lo_copy.start()

        @pl.when(k == 1)
        def _():
            for c, x, done in edges:
                face = jnp.where(spot64 >= 56, done[0], 0.0)
                for q in range(1, 4):
                    face = face + pltpu.roll(jnp.where(spot64 >= 56, done[q], 0.0), 128 - 8 * q, 1)
                hi_ref[c, x] = face

            @pl.when(gy < n_gy - 1)
            def _():
                hi_copy.start()

        return carry

    def inner(k, carry):
        ghost(k, carry)
        assembled(k)
        return carry

    def above(v):
        return jnp.where(spot64 >= 56, pltpu.roll(v, 56, 1), 0.0)

    def below(v):
        return jnp.where(spot64 < 8, pltpu.roll(v, 72, 1), 0.0)

    def across(c, carry):
        for x in range(exd):
            for q in range(4):
                spot = slice(q * 128, (q + 1) * 128)
                cells = [field_ref[c, x, y, :, spot] for y in range(eyd)]
                for y in range(eyd):
                    v = cells[y]
                    if y + 1 < eyd:
                        v = v + above(cells[y + 1])
                    if y > 0:
                        v = v + below(cells[y - 1])
                    field_ref[c, x, y, :, spot] = v
        return carry

    def edge(far_ref, y, keep, turn):
        for c in range(3):
            for x in range(exd):
                far_edge = far_ref[c, x]
                for q in range(4):
                    spot = slice(q * 128, (q + 1) * 128)
                    add = jnp.where(keep, pltpu.roll(far_edge, turn(q) % 128, 1), 0.0)
                    field_ref[c, x, y, :, spot] = field_ref[c, x, y, :, spot] + add

    def face_wait(at):
        for side in range(2):
            @pl.when(has[side])
            def _():
                face_copy(from_side, side, at).wait()

    lax.fori_loop(0, 2, ghost, 0)
    place_copy.wait()
    for m in order:
        back_copy(m).wait()
    lax.fori_loop(0, elems // 8, pick, 0)
    face_wait(0)
    lax.fori_loop(0, 2, outer, 0)
    for at in range(1, pairs):
        face_wait(at)
    lax.fori_loop(2, eyd, inner, 0)
    lax.fori_loop(0, 3, across, 0)
    for k in range(eyd):
        strip_sent(k)

    @pl.when(gy > 0)
    def _():
        hi_copy.wait_recv()
        edge(far_hi_ref, 0, spot64 < 8, lambda q: 72 + 8 * q)
        lo_copy.wait_send()

    @pl.when(gy < n_gy - 1)
    def _():
        lo_copy.wait_recv()
        edge(far_lo_ref, eyd - 1, spot64 >= 56, lambda q: 56 - 8 * q)
        hi_copy.wait_send()


def run_main(arrays, shape):
    exd, eyd, ez = shape
    elems = exd * eyd * ez
    columns = eyd * ez
    n_gx, n_gy = lax.axis_size("gx"), lax.axis_size("gy")
    f32, i32 = jnp.float32, jnp.int32
    dma = pltpu.SemaphoreType.DMA
    face = (3, exd, ez, 128)
    label = (n_gy, 1, 2 * elems)
    strips = (2, 3, columns, 128)
    hbm = [pltpu.with_memory_space_constraint(x, pltpu.HBM) for x in arrays]
    return pl.pallas_call(
        functools.partial(main_kernel, shape, n_gx, n_gy),
        out_shape=(
            jax.ShapeDtypeStruct((3, exd, eyd, ez, 512), f32),
            jax.ShapeDtypeStruct((3, elems, 128), f32),
        ),
        in_specs=[pl.BlockSpec(memory_space=pltpu.HBM)] * len(hbm),
        out_specs=[pl.BlockSpec(memory_space=VMEM)] * 2,
        scratch_shapes=[
            *(pltpu.VMEM(x.shape, x.dtype) for x in arrays),
            pltpu.VMEM(label, i32),
            pltpu.VMEM((1, elems), i32),
            pltpu.SMEM((1, elems), i32),
            pltpu.VMEM((3, elems, 128), f32),
            pltpu.VMEM((5, elems, 128), f32),
            pltpu.VMEM((3, elems, 128), f32),
            pltpu.VMEM((5, elems, 128), f32),
            pltpu.VMEM(label, i32),
            pltpu.VMEM((1, 128), i32),
            pltpu.SMEM(label, i32),
            pltpu.SMEM((1, 128), i32),
            pltpu.VMEM((elems * ROWS, 128), f32),
            pltpu.VMEM((3, elems, 128), f32),
            pltpu.VMEM((3, elems, 128), f32),
            pltpu.VMEM((elems * 2 * ROWS, 128), f32),
            pltpu.VMEM((elems * ROWS, 128), f32),
            pltpu.VMEM(strips, f32),
            pltpu.VMEM(strips, f32),
            pltpu.VMEM(strips, f32),
            pltpu.VMEM(strips, f32),
            pltpu.VMEM(strips, f32),
            pltpu.VMEM((2, 3, columns // 2, 128), f32),
            pltpu.VMEM((2, 3, columns // 2, 128), f32),
            pltpu.VMEM(face, f32),
            pltpu.VMEM(face, f32),
            pltpu.VMEM((3, elems, 128), f32),
            pltpu.VMEM((2, columns, 8, 128), f32),
            pltpu.VMEM((2, columns, 64, 256), jnp.bfloat16),
            pltpu.VMEM(face, f32),
            pltpu.VMEM(face, f32),
            dma((len(hbm),)),
            dma((2, n_gy - 1)),
            dma((2, n_gy - 1)),
            dma((2, n_gy - 1)),
            dma((n_gy + 2,)),
            dma((2, 2)),
            dma((2, 2, eyd)),
            dma((2, 2, eyd // 2)),
            dma((2, 2)),
            dma((2, n_gy - 1)),
        ],
        compiler_params=pltpu.CompilerParams(
            vmem_limit_bytes=40 * 1024 * 1024, collective_id=0, has_side_effects=True
        ),
        name="elements",
    )(*hbm)


def store_pass(field_ref, final_ref, out_ref, drag_ref, sem):
    copies = [pltpu.make_async_copy(field_ref.at[c], out_ref.at[c], sem.at[c]) for c in range(3)]
    copies.append(pltpu.make_async_copy(final_ref, drag_ref, sem.at[3]))
    for copy in copies:
        copy.start()
    for copy in copies:
        copy.wait()


def run_store(field, final):
    f32 = jnp.float32
    return pl.pallas_call(
        store_pass,
        out_shape=(jax.ShapeDtypeStruct(field.shape, f32), jax.ShapeDtypeStruct(final.shape, f32)),
        in_specs=[pl.BlockSpec(memory_space=VMEM)] * 2,
        out_specs=[pl.BlockSpec(memory_space=pl.ANY)] * 2,
        scratch_shapes=[pltpu.SemaphoreType.DMA((4,))],
        compiler_params=pltpu.CompilerParams(vmem_limit_bytes=32 * 1024 * 1024),
        name="store",
    )(field, final)


def body(velocity, part_pos, part_vel, part_coef, counts, dest, elem):
    _, exd, eyd, ez, nodes = velocity.shape
    elems = exd * eyd * ez
    arrays = (
        dest.reshape(1, elems), elem.reshape(1, elems), counts.reshape(1, elems),
        part_pos.transpose(1, 0, 2), part_vel.transpose(1, 0, 2), part_coef.reshape(2 * elems, 128),
        velocity.reshape(3, elems, nodes),
    )
    source, drag_out = run_store(*run_main(arrays, (exd, eyd, ez)))
    return (drag_out.transpose(1, 0, 2), source)


def solution(mesh):
    in_specs = (
        P(None, "gx", "gy", None, None),
        P(("gx", "gy"), None, None),
        P(("gx", "gy"), None, None),
        P(("gx", "gy"), None, None),
        P(("gx", "gy")),
        P(("gx", "gy")),
        P(("gx", "gy")),
    )
    out_specs = (P(("gx", "gy"), None, None), P(None, "gx", "gy", None, None))
    return jax.shard_map(body, mesh=mesh, in_specs=in_specs, out_specs=out_specs, check_vma=False)
```

```python
import functools
import math

import jax
import jax.numpy as jnp
from jax import lax
from jax.experimental import pallas as pl
from jax.experimental.pallas import tpu as pltpu
from jax.sharding import PartitionSpec as P

GLL = (
    -1.0,
    -0.8717401485096066,
    -0.5917001814331423,
    -0.2092992179024789,
    0.2092992179024789,
    0.5917001814331423,
    0.8717401485096066,
    1.0,
)
SHARPNESS = 8.0
WIDTH = math.sqrt(SHARPNESS * math.log2(math.e))
VMEM = pltpu.VMEM
SMEM = pltpu.SMEM
ROWS = 24


def lane_iota(shape):
    return lax.broadcasted_iota(jnp.int32, shape, len(shape) - 1)


def node_consts():
    row = lax.broadcasted_iota(jnp.int32, (8, 128), 0)

    def pick(values):
        out = jnp.full((8, 128), values[7], jnp.float32)
        for i in range(7):
            out = jnp.where(row == i, jnp.float32(values[i]), out)
        return out

    others = [pick([[GLL[m] for m in range(8) if m != i][n] for i in range(8)]) for n in range(7)]
    scales = []
    for i in range(8):
        product = 1.0
        for m in range(8):
            if m != i:
                product *= GLL[i] - GLL[m]
        scales.append(1.0 / product)
    return pick(GLL), others, pick(scales)


def lagrange(x, others, scale):
    diffs = [x - o for o in others]
    left = (diffs[0] * diffs[1]) * (diffs[2] * diffs[3])
    right = (diffs[4] * diffs[5]) * (diffs[6] * scale)
    return left * right


def gauss(x, nodes):
    gap = nodes - x
    return jnp.exp2(-(gap * gap))


def split(x):
    high = x.astype(jnp.bfloat16)
    low = (x - high.astype(jnp.float32)).astype(jnp.bfloat16)
    return high, low


def planes(a, b):
    return jnp.concatenate([a[j : j + 1] * b for j in range(8)], axis=0)


def spread_nodes(vel_ref, vs_ref, elems):
    low = lane_iota((elems, 128)) < 64
    for c in range(3):
        for q in range(4):
            x = vel_ref[c, :, q * 128 : (q + 1) * 128].astype(jnp.float32)
            turned = pltpu.roll(x, 64, 1)
            vs_ref[pl.ds(c * 8 + 2 * q, elems, stride=ROWS), :] = jnp.where(low, x, turned)
            vs_ref[pl.ds(c * 8 + 2 * q + 1, elems, stride=ROWS), :] = jnp.where(low, turned, x)


def rows_of(refs):
    return jnp.concatenate(refs, axis=0)


def project(left, both_planes):
    top, rest = split(left)
    both = jnp.concatenate([jnp.concatenate([top, top], axis=1), jnp.concatenate([rest, rest], axis=1)], axis=0)
    out = lax.dot_general(
        both, both_planes, (((1,), (1,)), ((), ())), preferred_element_type=jnp.float32
    )
    return out[: left.shape[0]] + out[left.shape[0] :]


def st_planes(s, t, nodes):
    return split(planes(gauss(s, nodes), gauss(t, nodes)))


def line(ref, c, at):
    return ref[c, pl.ds(at, 1), :]


def wide_line(ref, c, at):
    return jnp.broadcast_to(line(ref, c, at), (8, 128))


def main_kernel(
    shape, n_gx, n_gy,
    dest_hbm, elem_hbm, count_hbm, pos_hbm, vel_hbm, coef_hbm, velocity_hbm,
    field_ref, final_ref,
    dest_in, elem_in, count_in, pos_in, vel_in, coef_in, vel_ref, label_ref, place_row, position_ref, send_pos, send_rest, got_pos, got_rest, got_label, slot_row, tag_s, slot_s,
    vs_ref, fluid_ref, drag_ref, dep_ref, ts_ref, fs_ref,
    pos_ref, gpos_ref, out_ref, gdrag_ref, face_ref, gface_ref, lo_ref, hi_ref, ret_ref, weight_ref, plane_ref, far_lo_ref, far_hi_ref,
    in_sem, label_sem, block_sem, rest_sem, tag_sem, pos_sem, drag_sem, face_sem, y_sem, back_sem,
):
    exd, eyd, ez = shape
    elems = exd * eyd * ez
    columns = eyd * ez
    share = elems // n_gy
    group = 16
    per = share // group
    near = n_gy // 2
    i32 = jnp.int32
    gx = lax.axis_index("gx")
    gy = lax.axis_index("gy")
    has = (gx > 0, gx < n_gx - 1)
    mesh_id = pl.DeviceIdType.MESH

    def partner(m):
        total, bit = 0, 1
        while bit < n_gy:
            total = total + lax.rem(lax.div(gy, bit) + lax.div(m, bit), 2) * bit
            bit *= 2
        return total

    pairs = (
        (dest_hbm, dest_in), (elem_hbm, elem_in), (count_hbm, count_in),
        (pos_hbm, pos_in), (vel_hbm, vel_in), (coef_hbm, coef_in), (velocity_hbm, vel_ref),
    )
    inputs = [pltpu.make_async_copy(src, dst, in_sem.at[i]) for i, (src, dst) in enumerate(pairs)]
    for copy in inputs:
        copy.start()

    def side_id(side):
        return {"gx": gx - 1 if side == 0 else gx + 1}

    def to_side(side, src, dst, sems, *at):
        return pltpu.make_async_remote_copy(
            src_ref=src, dst_ref=dst, send_sem=sems.at[(0, side) + at], recv_sem=sems.at[(1, 1 - side) + at],
            device_id=side_id(side), device_id_type=mesh_id,
        )

    def from_side(side, src, dst, sems, *at):
        return pltpu.make_async_remote_copy(
            src_ref=src, dst_ref=dst, send_sem=sems.at[(0, side) + at], recv_sem=sems.at[(1, side) + at],
            device_id=side_id(side), device_id_type=mesh_id,
        )

    barrier = pltpu.get_barrier_semaphore()
    for side in range(2):
        @pl.when(has[side])
        def _():
            pl.semaphore_signal(barrier, inc=1, device_id=side_id(side), device_id_type=mesh_id)
    for m in range(1, n_gy):
        pl.semaphore_signal(barrier, inc=1, device_id={"gy": partner(m)}, device_id_type=mesh_id)

    def peer_copy(src, dst, sems, m):
        return pltpu.make_async_remote_copy(
            src_ref=src, dst_ref=dst, send_sem=sems.at[0, m - 1], recv_sem=sems.at[1, m - 1],
            device_id={"gy": partner(m)}, device_id_type=mesh_id,
        )

    def part(index):
        return pl.ds(pl.multiple_of(index * share, 8), share)

    def label_copy(m):
        return peer_copy(label_ref.at[partner(m)], got_label.at[gy], label_sem, m)

    def pos_copy(m):
        return peer_copy(send_pos.at[:, part(partner(m))], got_pos.at[:, part(gy)], block_sem, m)

    def rest_copy(m):
        return peer_copy(send_rest.at[:, part(partner(m))], got_rest.at[:, part(gy)], rest_sem, m)

    def back_copy(m):
        return peer_copy(drag_ref.at[:, part(partner(m))], ret_ref.at[:, part(gy)], back_sem, m)

    def tag_copy(index, m):
        return pltpu.make_async_copy(got_label.at[index], tag_s.at[index], tag_sem.at[m])

    @pl.when(gy == 0)
    def _():
        far_hi_ref[...] = jnp.zeros(far_hi_ref.shape, jnp.float32)

    @pl.when(gy == n_gy - 1)
    def _():
        far_lo_ref[...] = jnp.zeros(far_lo_ref.shape, jnp.float32)

    for side in range(2):
        @pl.when(jnp.logical_not(has[side]))
        def _():
            gpos_ref[side] = jnp.zeros(gpos_ref.shape[1:], jnp.float32)
            gdrag_ref[side] = jnp.zeros(gdrag_ref.shape[1:], jnp.float32)

    f32, bf16 = jnp.float32, jnp.bfloat16
    across_lanes = (((1,), (1,)), ((), ()))
    height = lax.broadcasted_iota(i32, (elems, elems), 0)
    for copy in inputs[:3]:
        copy.wait()
    dest_row, elem_row = dest_in[...], elem_in[...]
    square = (elems, elems)
    wide = lane_iota(square)

    def turned(x):
        return jnp.broadcast_to(x, square).T

    def summed(x):
        while x.shape[0] > 8:
            x = x[: x.shape[0] // 2] + x[x.shape[0] // 2 :]
        for step in (4, 2, 1):
            x = x + pltpu.roll(x, step, 0)
        return x[0:1]

    dest_col, elem_col = turned(dest_row), turned(elem_row)
    rank = summed(jnp.where((dest_col == dest_row) & (height < wide), 1, 0))
    place = dest_row * share + rank
    place_row[...] = place
    place_copy = pltpu.make_async_copy(place_row, position_ref, tag_sem.at[n_gy + 1])
    place_copy.start()
    chosen = (place == height).astype(bf16)
    place_col = turned(place)
    tags = summed(jnp.where(place_col == wide, elem_col, 0))
    slot_col = place_col + (gy - dest_col) * share
    slot_col = jnp.where(elem_col == wide, slot_col, 0)
    for d in range(n_gy):
        label_ref[d] = jnp.concatenate([tags, summed(jnp.where(dest_col == d, slot_col, 0))], axis=1)

    def picked(chosen, x):
        top = x.astype(bf16)
        left = x - top.astype(f32)
        middle = left.astype(bf16)
        bottom = (left - middle.astype(f32)).astype(bf16)
        return (
            jnp.dot(chosen, top, preferred_element_type=f32)
            + jnp.dot(chosen, middle, preferred_element_type=f32)
            + jnp.dot(chosen, bottom, preferred_element_type=f32)
        )

    order = tuple(range(near, n_gy)) + tuple(range(1, near))
    inputs[3].wait()
    both = picked(chosen, jnp.concatenate([pos_in[0], pos_in[1]], axis=1))
    send_pos[0] = both[:, :128]
    send_pos[1] = both[:, 128:]
    send_pos[2] = picked(chosen, pos_in[2])
    pl.semaphore_wait(barrier, n_gy - 1 + has[0].astype(i32) + has[1].astype(i32))
    for m in order:
        label_copy(m).start()
    for m in order:
        pos_copy(m).start()
    got_label[gy] = label_ref[gy]
    tag_copy(gy, 0).start()
    got_pos[:, part(gy), :] = send_pos[:, part(gy), :]
    inputs[4].wait()
    inputs[5].wait()
    both = picked(chosen, jnp.concatenate([vel_in[0], vel_in[1]], axis=1))
    send_rest[0] = both[:, :128]
    send_rest[1] = both[:, 128:]
    both = picked(chosen, jnp.concatenate([vel_in[2], coef_in[pl.ds(0, elems, stride=2), :]], axis=1))
    live = lax.dot_general(
        chosen, jnp.broadcast_to(count_in[...].astype(f32), (128, elems)).astype(bf16), across_lanes,
        preferred_element_type=f32,
    )
    send_rest[2] = both[:, :128]
    send_rest[3] = jnp.where(lane_iota((elems, 128)).astype(f32) < live, both[:, 128:], 0.0)
    send_rest[4] = picked(chosen, coef_in[pl.ds(1, elems, stride=2), :])
    for m in range(1, near):
        rest_copy(m).start()
    got_rest[:, part(gy), :] = send_rest[:, part(gy), :]
    inputs[6].wait()
    spread_nodes(vel_ref, vs_ref, elems)
    consts = node_consts()
    nodes, others, scale = consts
    nodes = nodes * WIDTH
    tag_copy(gy, 0).wait()

    def within(i):
        return jnp.minimum(jnp.maximum(i, 0), elems - 1)

    base = (0, elems - columns)

    def slot_of(e):
        return within(slot_s[0, e])

    def collect(dst, src, start, count):
        def some(i, carry):
            for side in range(2):
                at = pl.multiple_of(start + i * 8, 8)
                spots = [slot_of(side * columns + at + u) for u in range(8)]
                for c in range(3):
                    dst[side, c, pl.ds(at, 8), :] = rows_of([line(src, c, b) for b in spots])
            return carry

        lax.fori_loop(0, count // 8, some, 0)

    slot_copy = pltpu.make_async_copy(slot_row, slot_s, tag_sem.at[n_gy])

    def forces(start, count):
        def some(i, carry):
            m = lax.div(start + i * 8, share)
            at = pl.ds(pl.multiple_of(partner(m) * share + lax.rem(start + i * 8, share), 8), 8)
            rel = [fluid_ref[c, at, :] - got_rest[c, at, :] for c in range(3)]
            speed = jnp.sqrt(rel[0] * rel[0] + rel[1] * rel[1] + rel[2] * rel[2])
            power = jnp.exp(0.687 * jnp.log(got_rest[4, at, :] * speed))
            factor = got_rest[3, at, :] * (1.0 + 0.15 * power)
            for c in range(3):
                drag_ref[c, at, :] = factor * rel[c]
            return carry

        lax.fori_loop(0, count // 8, some, 0)

    def deposit_step(index, carry):
        source = partner(lax.div(index, per))
        first = lax.rem(index, per) * group
        for u in range(group):
            i = first + u
            slot = source * share + i
            layer = jnp.full((8, 128), tag_s[source, 0, gy * share + i], i32)
            shift = jnp.where(layer < columns, -2.0 * WIDTH, 2.0 * WIDTH)
            r, s, t = (wide_line(got_pos, d, slot) * WIDTH for d in range(3))
            weights = (gauss(r, nodes), gauss(r + shift, nodes))
            force = [-line(drag_ref, c, slot) for c in range(3)]
            left = jnp.concatenate([f * w for w in weights for f in force], axis=0)
            out = project(left, jnp.concatenate(st_planes(s, t, nodes), axis=1))
            dep_ref[pl.ds(pl.multiple_of(slot * 2 * ROWS, 8), 2 * ROWS), 0:64] = out
        return carry

    def interpolate(index, carry):
        @pl.when(index == per)
        def _():
            forces(0, share)
            lax.fori_loop(0, per, deposit_step, 0)
            for m in range(near, n_gy):
                pos_copy(m).wait_send()
                rest_copy(m).start()
            for m in order:
                label_copy(m).wait()
            total = got_label[0]
            for other in range(1, n_gy):
                total = total + got_label[other]
            slot_row[...] = total[:, elems:]
            slot_copy.start()
            for m in order:
                tag_copy(partner(m), m).start()
            wanted = (turned(total[:, elems:]) == wide).astype(bf16)
            for m in range(1, near):
                pos_copy(m).wait()
            for m in range(near, n_gy):
                pos_copy(m).wait_recv()
            for c in range(3):
                held = picked(wanted, got_pos[c])
                for side in range(2):
                    pos_ref[side, c] = held[base[side] : base[side] + columns]
            for side in range(2):
                @pl.when(has[side])
                def _():
                    to_side(side, pos_ref.at[side], gpos_ref.at[1 - side], pos_sem).start()
            slot_copy.wait()
            for m in order:
                tag_copy(partner(m), m).wait()

        source = partner(lax.div(index, per))
        first = lax.rem(index, per) * group
        for batch in range(group // 8):
            fluid = [[], [], []]
            for u in range(8):
                i = first + batch * 8 + u
                slot = source * share + i
                e = within(tag_s[source, 0, gy * share + i])
                r, s, t = (wide_line(got_pos, d, slot) for d in range(3))
                basis_r = lagrange(r, others, scale)
                high, low = split(planes(lagrange(s, others, scale), lagrange(t, others, scale)))
                partial = jnp.dot(
                    vs_ref[pl.ds(e * ROWS, ROWS), :].astype(jnp.bfloat16),
                    jnp.concatenate([high, low], axis=0),
                    preferred_element_type=jnp.float32,
                )
                for c in range(3):
                    fluid[c].append(jnp.sum(partial[c * 8 : c * 8 + 8] * basis_r, axis=0, keepdims=True))
            at = pl.multiple_of(source * share + first + batch * 8, 8)
            for c in range(3):
                fluid_ref[c, pl.ds(at, 8), :] = rows_of(fluid[c])
        return carry

    lax.fori_loop(0, elems // group, interpolate, 0)

    def strip(k):
        odd = lax.rem(k, 2)
        return odd * (eyd - 1) + (1 - 2 * odd) * lax.div(k, 2)

    def drag_copy(make, side, y):
        at = pl.ds(pl.multiple_of(y * ez, 8), ez)
        return make(side, out_ref.at[side, :, at], gdrag_ref.at[1 - side, :, at], drag_sem, y)

    def strip_start(k):
        for side in range(2):
            @pl.when(has[side])
            def _():
                drag_copy(to_side, side, strip(k)).start()

    def strip_sent(k):
        for side in range(2):
            @pl.when(has[side])
            def _():
                drag_copy(to_side, side, strip(k)).wait_send()

    def deposit(index, carry):
        @pl.when(index == per)
        def _():
            for m in range(1, near):
                rest_copy(m).wait()
            forces(share, (near - 1) * share)

        @pl.when(index == near * per)
        def _():
            for m in range(near, n_gy):
                rest_copy(m).wait()
            forces(near * share, elems - near * share)
            collect(out_ref, drag_ref, 0, columns)
            for k in range(2):
                strip_start(k)
            for m in order:
                back_copy(m).start()
            ret_ref[:, part(gy), :] = drag_ref[:, part(gy), :]

        return deposit_step(index, carry)

    lax.fori_loop(per, elems // group, deposit, 0)

    def gather(i, carry):
        for side in range(exd):
            spots = []
            for u in range(8):
                col = i * 8 + u
                mine = slot_of(side * columns + col) * (2 * ROWS)
                other = slot_of((1 - side) * columns + col) * (2 * ROWS) + ROWS
                e = side * columns + col
                ts_ref[pl.ds(pl.multiple_of(e * ROWS, 8), ROWS), :] = (
                    dep_ref[pl.ds(mine, ROWS), :] + dep_ref[pl.ds(other, ROWS), :]
                )
                spots.append(mine)
            node = 0 if side == 0 else 7
            for c in range(3):
                fs_ref[side, c, pl.ds(pl.multiple_of(i * 8, 8), 8), :] = rows_of(
                    [dep_ref[pl.ds(at + c * 8 + node, 1), :] for at in spots]
                )
        return carry

    lax.fori_loop(0, columns // 8, gather, 0)

    low = lane_iota((ez, 128)) < 64
    pairs = eyd // 2

    def face_copy(make, side, at):
        rows = pl.ds(pl.multiple_of(at * ez, 8), ez)
        there = 1 - side if make is to_side else side
        return make(side, face_ref.at[side, :, rows], gface_ref.at[there, :, rows], face_sem, at)

    for at in range(pairs):
        for side in range(2):
            node = 0 if side == 0 else 7
            for c in range(3):
                one = ts_ref[pl.ds((base[side] + at * ez) * ROWS + c * 8 + node, ez, stride=ROWS), :]
                two = ts_ref[pl.ds((base[side] + (eyd - 1 - at) * ez) * ROWS + c * 8 + node, ez, stride=ROWS), :]
                face_ref[side, c, at * ez : (at + 1) * ez, :] = jnp.where(low, one, pltpu.roll(two, 64, 1))
    for at in range(pairs):
        for side in range(2):
            @pl.when(has[side])
            def _():
                face_copy(to_side, side, at).start()
    for k in range(2, eyd):
        strip_start(k)

    for side in range(2):
        @pl.when(has[side])
        def _():
            from_side(side, pos_ref.at[side], gpos_ref.at[side], pos_sem).wait()

    def prepare(k, carry):
        for side in range(2):
            for g in range(8):
                col = k * 8 + g
                r, s, t = (jnp.broadcast_to(gpos_ref[side, d, pl.ds(col, 1), :], (8, 128)) * WIDTH for d in range(3))
                weight_ref[side, col] = gauss(r + (-2.0 if side == 0 else 2.0) * WIDTH, nodes)
                plane_ref[side, col] = jnp.concatenate(st_planes(s, t, nodes), axis=1)
        return carry

    lax.fori_loop(0, columns // 8, prepare, 0)

    def pick(i, carry):
        at = pl.multiple_of(i * 8, 8)
        spots = [within(position_ref[0, at + u]) for u in range(8)]
        for c in range(3):
            final_ref[c, pl.ds(at, 8), :] = rows_of([line(ret_ref, c, spot) for spot in spots])
        return carry


    def ghost(k, carry):
        y = strip(k)
        at = pl.ds(pl.multiple_of(y * ez, 8), ez)
        for side in range(2):
            @pl.when(has[side])
            def _():
                from_side(side, out_ref.at[side, :, at], gdrag_ref.at[side, :, at], drag_sem, y).wait_recv()
        sums = []
        for side in range(2):
            for g in range(ez):
                col = y * ez + g
                weight = weight_ref[side, col]
                left = jnp.concatenate([(-gdrag_ref[side, c, pl.ds(col, 1), :]) * weight for c in range(3)], axis=0)
                add = project(left, plane_ref[side, col])
                spot = pl.ds(pl.multiple_of((base[side] + col) * ROWS, 8), ROWS)
                sums.append((spot, ts_ref[spot, 0:64] + add))
        for spot, value in sums:
            ts_ref[spot, 0:64] = value
        return carry

    spot64 = lane_iota((ez, 128)) % 64
    depth = lax.broadcasted_iota(jnp.int32, (ez, 128), 0)
    up = (spot64 % 8 == 7) & (depth < ez - 1)
    down = (spot64 % 8 == 0) & (depth > 0)
    lo_copy = pltpu.make_async_remote_copy(
        src_ref=lo_ref, dst_ref=far_lo_ref, send_sem=y_sem.at[0, 0], recv_sem=y_sem.at[1, 0],
        device_id={"gy": gy - 1}, device_id_type=mesh_id,
    )
    hi_copy = pltpu.make_async_remote_copy(
        src_ref=hi_ref, dst_ref=far_hi_ref, send_sem=y_sem.at[0, 1], recv_sem=y_sem.at[1, 1],
        device_id={"gy": gy + 1}, device_id_type=mesh_id,
    )

    def through(v):
        nxt = pltpu.roll(pltpu.roll(v, ez - 1, 0), 7, 1)
        prv = pltpu.roll(pltpu.roll(v, 1, 0), 121, 1)
        return v + jnp.where(up, nxt, 0.0) + jnp.where(down, prv, 0.0)

    def lanes(c, x, y, q):
        start = (x * columns + y * ez) * ROWS + c * 8 + 2 * q
        even = ts_ref[pl.ds(start, ez, stride=ROWS), :]
        odd = ts_ref[pl.ds(start + 1, ez, stride=ROWS), :]
        return jnp.where(low, even, pltpu.roll(odd, 64, 1))

    def far(c, side, y, at, upper):
        came = gface_ref[side, c, pl.ds(pl.multiple_of(at * ez, 8), ez), :]
        turn = pltpu.roll(came, 64, 1)
        came = jnp.where(low != upper, came, turn)
        mine = fs_ref[side, c, pl.ds(pl.multiple_of(y * ez, 8), ez), :]
        mine = jnp.where(low, mine, pltpu.roll(mine, 64, 1))
        return jnp.where(has[side] & (low if side == 0 else jnp.logical_not(low)), came + mine, 0.0)

    def assembled(k):
        y = strip(k)
        out = []
        for c in range(3):
            grid = [[lanes(c, x, y, q) for q in range(4)] for x in range(exd)]
            for x in range(exd):
                done = list(grid[x])
                if x + 1 < exd:
                    done[3] = done[3] + jnp.where(low, 0.0, pltpu.roll(grid[x + 1][0], 64, 1))
                else:
                    done[3] = done[3] + far(c, 1, y, lax.div(k, 2), lax.rem(k, 2) == 1)
                if x > 0:
                    done[0] = done[0] + jnp.where(low, pltpu.roll(grid[x - 1][3], 64, 1), 0.0)
                else:
                    done[0] = done[0] + far(c, 0, y, lax.div(k, 2), lax.rem(k, 2) == 1)
                done = [through(v) for v in done]
                for q in range(4):
                    field_ref[c, x, y, :, q * 128 : (q + 1) * 128] = done[q]
                out.append((c, x, done))
        return out

    def outer(k, carry):
        edges = assembled(k)

        @pl.when(k == 0)
        def _():
            for c, x, done in edges:
                face = jnp.where(spot64 < 8, done[0], 0.0)
                for q in range(1, 4):
                    face = face + pltpu.roll(jnp.where(spot64 < 8, done[q], 0.0), 8 * q, 1)
                lo_ref[c] = face if x == 0 else lo_ref[c] + pltpu.roll(face, 32 * x, 1)

            @pl.when(gy > 0)
            def _():
                lo_copy.start()

        @pl.when(k == 1)
        def _():
            for c, x, done in edges:
                face = jnp.where(spot64 >= 56, done[0], 0.0)
                for q in range(1, 4):
                    face = face + pltpu.roll(jnp.where(spot64 >= 56, done[q], 0.0), 128 - 8 * q, 1)
                hi_ref[c] = face if x == 0 else hi_ref[c] + pltpu.roll(face, 32 * x, 1)

            @pl.when(gy < n_gy - 1)
            def _():
                hi_copy.start()

        return carry

    def inner(k, carry):
        ghost(k, carry)
        assembled(k)
        return carry

    def above(v):
        return jnp.where(spot64 >= 56, pltpu.roll(v, 56, 1), 0.0)

    def below(v):
        return jnp.where(spot64 < 8, pltpu.roll(v, 72, 1), 0.0)

    def across(c, carry):
        for x in range(exd):
            for q in range(4):
                spot = slice(q * 128, (q + 1) * 128)
                cells = [field_ref[c, x, y, :, spot] for y in range(eyd)]
                for y in range(eyd):
                    v = cells[y]
                    if y + 1 < eyd:
                        v = v + above(cells[y + 1])
                    if y > 0:
                        v = v + below(cells[y - 1])
                    field_ref[c, x, y, :, spot] = v
        return carry

    def edges_in(c, carry):
        for x in range(exd):
            hi, lo = far_hi_ref[c], far_lo_ref[c]
            for q in range(4):
                spot = slice(q * 128, (q + 1) * 128)
                add = jnp.where(spot64 < 8, pltpu.roll(hi, (72 + 8 * q - 32 * x) % 128, 1), 0.0)
                field_ref[c, x, 0, :, spot] = field_ref[c, x, 0, :, spot] + add
                add = jnp.where(spot64 >= 56, pltpu.roll(lo, (56 - 8 * q - 32 * x) % 128, 1), 0.0)
                field_ref[c, x, eyd - 1, :, spot] = field_ref[c, x, eyd - 1, :, spot] + add
        return carry

    def face_wait(at):
        for side in range(2):
            @pl.when(has[side])
            def _():
                face_copy(from_side, side, at).wait()

    place_copy.wait()
    for m in order:
        back_copy(m).wait()
    lax.fori_loop(0, elems // 8, pick, 0)
    lax.fori_loop(0, 2, ghost, 0)
    face_wait(0)
    lax.fori_loop(0, 2, outer, 0)
    for at in range(1, pairs):
        face_wait(at)
    lax.fori_loop(2, eyd, inner, 0)
    lax.fori_loop(0, 3, across, 0)
    for k in range(eyd):
        strip_sent(k)

    @pl.when(gy > 0)
    def _():
        hi_copy.wait_recv()
        lo_copy.wait_send()

    @pl.when(gy < n_gy - 1)
    def _():
        lo_copy.wait_recv()
        hi_copy.wait_send()

    lax.fori_loop(0, 3, edges_in, 0)


def run_main(arrays, shape):
    exd, eyd, ez = shape
    elems = exd * eyd * ez
    columns = eyd * ez
    n_gx, n_gy = lax.axis_size("gx"), lax.axis_size("gy")
    f32, i32 = jnp.float32, jnp.int32
    dma = pltpu.SemaphoreType.DMA
    face = (3, ez, 128)
    label = (n_gy, 1, 2 * elems)
    strips = (2, 3, columns, 128)
    hbm = [pltpu.with_memory_space_constraint(x, pltpu.HBM) for x in arrays]
    return pl.pallas_call(
        functools.partial(main_kernel, shape, n_gx, n_gy),
        out_shape=(
            jax.ShapeDtypeStruct((3, exd, eyd, ez, 512), f32),
            jax.ShapeDtypeStruct((3, elems, 128), f32),
        ),
        in_specs=[pl.BlockSpec(memory_space=pltpu.HBM)] * len(hbm),
        out_specs=[pl.BlockSpec(memory_space=VMEM)] * 2,
        scratch_shapes=[
            *(pltpu.VMEM(x.shape, x.dtype) for x in arrays),
            pltpu.VMEM(label, i32),
            pltpu.VMEM((1, elems), i32),
            pltpu.SMEM((1, elems), i32),
            pltpu.VMEM((3, elems, 128), f32),
            pltpu.VMEM((5, elems, 128), f32),
            pltpu.VMEM((3, elems, 128), f32),
            pltpu.VMEM((5, elems, 128), f32),
            pltpu.VMEM(label, i32),
            pltpu.VMEM((1, 128), i32),
            pltpu.SMEM(label, i32),
            pltpu.SMEM((1, 128), i32),
            pltpu.VMEM((elems * ROWS, 128), f32),
            pltpu.VMEM((3, elems, 128), f32),
            pltpu.VMEM((3, elems, 128), f32),
            pltpu.VMEM((elems * 2 * ROWS, 128), f32),
            pltpu.VMEM((elems * ROWS, 128), f32),
            pltpu.VMEM(strips, f32),
            pltpu.VMEM(strips, f32),
            pltpu.VMEM(strips, f32),
            pltpu.VMEM(strips, f32),
            pltpu.VMEM(strips, f32),
            pltpu.VMEM((2, 3, columns // 2, 128), f32),
            pltpu.VMEM((2, 3, columns // 2, 128), f32),
            pltpu.VMEM(face, f32),
            pltpu.VMEM(face, f32),
            pltpu.VMEM((3, elems, 128), f32),
            pltpu.VMEM((2, columns, 8, 128), f32),
            pltpu.VMEM((2, columns, 64, 256), jnp.bfloat16),
            pltpu.VMEM(face, f32),
            pltpu.VMEM(face, f32),
            dma((len(hbm),)),
            dma((2, n_gy - 1)),
            dma((2, n_gy - 1)),
            dma((2, n_gy - 1)),
            dma((n_gy + 2,)),
            dma((2, 2)),
            dma((2, 2, eyd)),
            dma((2, 2, eyd // 2)),
            dma((2, 2)),
            dma((2, n_gy - 1)),
        ],
        compiler_params=pltpu.CompilerParams(
            vmem_limit_bytes=40 * 1024 * 1024, collective_id=0, has_side_effects=True
        ),
        name="elements",
    )(*hbm)


def store_pass(field_ref, final_ref, out_ref, drag_ref, sem):
    copies = [pltpu.make_async_copy(field_ref.at[c], out_ref.at[c], sem.at[c]) for c in range(3)]
    copies.append(pltpu.make_async_copy(final_ref, drag_ref, sem.at[3]))
    for copy in copies:
        copy.start()
    for copy in copies:
        copy.wait()


def run_store(field, final):
    f32 = jnp.float32
    return pl.pallas_call(
        store_pass,
        out_shape=(jax.ShapeDtypeStruct(field.shape, f32), jax.ShapeDtypeStruct(final.shape, f32)),
        in_specs=[pl.BlockSpec(memory_space=VMEM)] * 2,
        out_specs=[pl.BlockSpec(memory_space=pl.ANY)] * 2,
        scratch_shapes=[pltpu.SemaphoreType.DMA((4,))],
        compiler_params=pltpu.CompilerParams(vmem_limit_bytes=32 * 1024 * 1024),
        name="store",
    )(field, final)


def body(velocity, part_pos, part_vel, part_coef, counts, dest, elem):
    _, exd, eyd, ez, nodes = velocity.shape
    elems = exd * eyd * ez
    arrays = (
        dest.reshape(1, elems), elem.reshape(1, elems), counts.reshape(1, elems),
        part_pos.transpose(1, 0, 2), part_vel.transpose(1, 0, 2), part_coef.reshape(2 * elems, 128),
        velocity.reshape(3, elems, nodes),
    )
    source, drag_out = run_store(*run_main(arrays, (exd, eyd, ez)))
    return (drag_out.transpose(1, 0, 2), source)


def solution(mesh):
    in_specs = (
        P(None, "gx", "gy", None, None),
        P(("gx", "gy"), None, None),
        P(("gx", "gy"), None, None),
        P(("gx", "gy"), None, None),
        P(("gx", "gy")),
        P(("gx", "gy")),
        P(("gx", "gy")),
    )
    out_specs = (P(("gx", "gy"), None, None), P(None, "gx", "gy", None, None))
    return jax.shard_map(body, mesh=mesh, in_specs=in_specs, out_specs=out_specs, check_vma=False)
```
